32 devices in a mesh: dp: 4 (over x, core), ctx: 8 (over z, y).
Axes of the slice: x: 2, y: 2, z: 4, core: 2. Of those that a mesh axis runs over, the one named last changes fastest.
Arguments:
- density: float32 [128, 64, 64], P(('dp', 'ctx')), parts along dimension 0, may hold values from 0.1 to 50, as said below
- stem_weight: bfloat16 [216, 1024], replicated, may hold values from -0.4375 to 0.4375
- stem_bias: float32 [1024], replicated, may hold values from -3 to 3
- pos_embed: bfloat16 [2048, 1024], P('ctx'), may hold values from -3 to 3
- ln1_gain: float32 [1024], replicated, may hold values from 0.25 to 1.75
- ln1_bias: float32 [1024], replicated, may hold values from -2 to 2
- w_qkv: bfloat16 [1024, 3072], replicated, may hold values from -2 to 2
- qkv_bias: float32 [3072], replicated, may hold values from -2 to 2
- w_out: bfloat16 [1024, 1024], replicated, may hold values from -0.1875 to 0.1875
- out_bias: float32 [1024], replicated, may hold values from -2 to 2
- ln2_gain: float32 [1024], replicated, may hold values from 0.25 to 1.75
- ln2_bias: float32 [1024], replicated, may hold values from -2 to 2
- w_fc1: bfloat16 [1024, 4096], replicated, may hold values from -0.1875 to 0.1875
- fc1_bias: float32 [4096], replicated, may hold values from -3 to 3
- w_fc2: bfloat16 [4096, 1024], replicated, may hold values from -0.09375 to 0.09375
- fc2_bias: float32 [1024], replicated, may hold values from -2 to 2
Outputs:
- encoded: bfloat16 [8192, 1024], P(('dp', 'ctx')), parts along dimension 0
The draws below stay inside these ranges and needn't reach their ends.
There are 4 independent parts, one for each index of `dp`. The reference program is written for one: setup_inputs(seed, part) draws one part's arguments, and reference() takes and returns one part's arrays. A program takes and returns all parts, laid end to end along the dimension named above; an argument that names none is the same for every part. Nothing has to cross between parts.
Inputs may be any that keep to these rules, and one draw needn't show every extreme that they name: density is positive.
All inputs are finite; a program needn't handle non-finite values.
Results may differ from the reference program's by a relative error of at most 0.013.
Values may be sent and summed in bfloat16 or wider, within the bound.
A program may use at most 384 MiB of HBM per device.

```python
import math
import jax
import jax.numpy as jnp
from jax import lax

D = 1024
FF = 4096
HEADS = 16
KERNEL = 6
STRIDE = 4
GYZ = 16
TX = 8
TOKENS = 2048


def draw_density(key, part):
    planes = STRIDE * TX
    side_cells = STRIDE * GYZ
    key_one = jax.random.fold_in(key, 11)
    gradient = jnp.arange(planes, dtype=jnp.float32)[:, None, None] / max(planes - 1, 1)
    entries = jnp.exp(jax.random.uniform(key_one, (planes, side_cells, side_cells), jnp.float32, math.log(0.2), math.log(5.0)))
    scaling = jnp.exp(math.log(3.0) * gradient)
    return entries * scaling


def draw_w_qkv(key, part):
    key_one = jax.random.fold_in(jax.random.fold_in(key, 23), 0)
    spread = 1.6 / math.sqrt(D)
    return (jnp.clip(jax.random.normal(key_one, (D, 3 * D), jnp.float32), -6.0, 6.0) * spread).astype(jnp.bfloat16)


def block_scale(stream_key, extent, shards, low, top_value):
    def one(position, parts):
        draws = jax.random.uniform(jax.random.fold_in(jax.random.fold_in(stream_key, 6), position), (parts,), jnp.float32, low / len(shards), top_value / len(shards))
        return jnp.repeat(jnp.exp(draws), extent[position] // parts).reshape((-1,) + (1,) * (len(extent) - position - 1))

    level = one(*shards[0])
    for cut in shards[1:]:
        level = level * one(*cut)
    return level


def scatter_about(key, extent, scale, most, cuts=(), kind=jnp.bfloat16):
    gain = block_scale(key, extent, cuts, -0.22, 0.18) if cuts else 1.0
    values = jax.random.normal(key, extent, jnp.float32) * scale * gain
    return jnp.minimum(jnp.maximum(values, -most), most).astype(kind)


def setup_inputs(seed: int = 0, part: int = 0) -> dict:
    key_list = jax.random.split(jax.random.key(seed), 17)
    part_keys = jax.random.split(jax.random.fold_in(key_list[16], part), 17)
    return {
        "density": draw_density(jax.random.fold_in(jax.random.fold_in(key_list[16], part), 71), part),
        "stem_weight": scatter_about(key_list[1], (KERNEL * KERNEL * KERNEL, D), (KERNEL * KERNEL * KERNEL) ** -0.5, 0.4375),
        "stem_bias": scatter_about(key_list[2], (D,), 0.5, 3.0, (), jnp.float32),
        "pos_embed": scatter_about(key_list[3], (TOKENS, D), 0.5, 3.0, ((0, 8),)),
        "ln1_gain": jnp.clip(1.0 + 0.15 * jax.random.normal(key_list[4], (D,), jnp.float32), 0.25, 1.75),
        "ln1_bias": scatter_about(key_list[5], (D,), 0.3, 2.0, (), jnp.float32),
        "w_qkv": draw_w_qkv(jax.random.fold_in(key_list[16], 71), part),
        "qkv_bias": scatter_about(key_list[7], (3 * D,), 0.3, 2.0, (), jnp.float32),
        "w_out": scatter_about(key_list[8], (D, D), D ** -0.5, 0.1875),
        "out_bias": scatter_about(key_list[9], (D,), 0.3, 2.0, (), jnp.float32),
        "ln2_gain": jnp.clip(1.0 + 0.15 * jax.random.normal(key_list[10], (D,), jnp.float32), 0.25, 1.75),
        "ln2_bias": scatter_about(key_list[11], (D,), 0.3, 2.0, (), jnp.float32),
        "w_fc1": scatter_about(key_list[12], (D, FF), D ** -0.5, 0.1875),
        "fc1_bias": scatter_about(key_list[13], (FF,), 0.5, 3.0, (), jnp.float32),
        "w_fc2": scatter_about(key_list[14], (FF, D), FF ** -0.5, 0.09375),
        "fc2_bias": scatter_about(key_list[15], (D,), 0.3, 2.0, (), jnp.float32),
    }


def layer_norm(inputs, gain_vector, shift_vector):
    values = inputs.astype(jnp.float32)
    center = values - lax.optimization_barrier(jnp.mean(values, axis=-1, keepdims=True))
    spread = lax.optimization_barrier(jnp.mean(center * center, axis=-1, keepdims=True))
    return center * lax.rsqrt(spread + 1e-06) * gain_vector + shift_vector

def stem_conv(stacked, stem_weight):
    model_width = stem_weight.shape[1]
    kernel = stem_weight.reshape(6, 6, 6, 1, model_width)
    result = lax.conv_general_dilated(stacked[..., None], kernel, (4, 4, 4), ((1, 1), (1, 1), (1, 1)), dimension_numbers=('NDHWC', 'DHWIO', 'NDHWC'), preferred_element_type=jnp.float32)
    return result.reshape(-1, model_width)

def single_head(triple):
    query_head, key_head, value_head = triple
    scores = jnp.dot(query_head, key_head.T, preferred_element_type=jnp.float32)
    row_max = lax.optimization_barrier(jnp.max(scores, axis=1, keepdims=True))
    weights = jnp.exp(scores - row_max)
    row_total = lax.optimization_barrier(jnp.sum(weights, axis=1, keepdims=True))
    mixed = jnp.dot(weights.astype(jnp.bfloat16), value_head, preferred_element_type=jnp.float32) / row_total
    return mixed.astype(jnp.bfloat16)

def reference(density, stem_weight, stem_bias, pos_embed, ln1_gain, ln1_bias, w_qkv, qkv_bias, w_out, out_bias, ln2_gain, ln2_bias, w_fc1, fc1_bias, w_fc2, fc2_bias):
    model_width = w_out.shape[0]
    head_size = model_width // HEADS
    mean_density = jnp.mean(density)
    field = jnp.log(density / mean_density).astype(jnp.bfloat16)
    embedded = stem_conv(field[None], stem_weight) + stem_bias + pos_embed.astype(jnp.float32)
    residual = embedded.astype(jnp.bfloat16)
    normed = layer_norm(residual, ln1_gain, ln1_bias).astype(jnp.bfloat16)
    projected = jnp.dot(normed, w_qkv, preferred_element_type=jnp.float32) + qkv_bias
    token_count = normed.shape[0]
    query_rows = (projected[:, :model_width] * (1.0 / head_size ** 0.5)).astype(jnp.bfloat16)
    key_rows = projected[:, model_width:2 * model_width].astype(jnp.bfloat16)
    value_rows = projected[:, 2 * model_width:].astype(jnp.bfloat16)

    def split_heads(matrix):
        return matrix.reshape(token_count, HEADS, head_size).transpose(1, 0, 2)
    attended = lax.map(single_head, (split_heads(query_rows), split_heads(key_rows), split_heads(value_rows)))
    attended = attended.transpose(1, 0, 2).reshape(token_count, model_width)
    stream = (residual.astype(jnp.float32) + jnp.dot(attended, w_out, preferred_element_type=jnp.float32) + out_bias).astype(jnp.bfloat16)
    normed_two = layer_norm(stream, ln2_gain, ln2_bias).astype(jnp.bfloat16)
    hidden = jax.nn.gelu(jnp.dot(normed_two, w_fc1, preferred_element_type=jnp.float32) + fc1_bias, approximate=False).astype(jnp.bfloat16)
    encoded = stream.astype(jnp.float32) + jnp.dot(hidden, w_fc2, preferred_element_type=jnp.float32) + fc2_bias
    return encoded.astype(jnp.bfloat16)
```

```python
import functools
import math

import jax
import jax.numpy as jnp
import numpy as np
from jax import lax
from jax.experimental import pallas as pl
from jax.experimental.pallas import tpu as pltpu
from jax.sharding import PartitionSpec as P

HEADS = 16
KERNEL = 6
STRIDE = 4
ROWS = 128
MESH = pl.DeviceIdType.MESH
F32 = jnp.float32
BF16 = jnp.bfloat16


def iota(shape, axis):
    return lax.broadcasted_iota(jnp.int32, shape, axis)


def partner(me, mask, n):
    result, bit = 0, 1
    while bit < n:
        result += ((me // bit + mask // bit) % 2) * bit
        bit *= 2
    return result


def norm_rows(values, gain_vector, shift_vector):
    center = values - jnp.mean(values, axis=-1, keepdims=True)
    spread = jnp.mean(center * center, axis=-1, keepdims=True)
    return center * lax.rsqrt(spread + 1e-06) * gain_vector + shift_vector


def layer_kernel(
    n,
    cells,
    density,
    stem_weight,
    stem_bias,
    pos_embed,
    ln1_gain,
    ln1_bias,
    w_qkv_hbm,
    qkv_bias,
    w_out_hbm,
    out_bias,
    ln2_gain,
    ln2_bias,
    w_fc1_hbm,
    fc1_bias,
    w_fc2_hbm,
    fc2_bias,
    encoded,
    w_qkv,
    w_out,
    w_fc1,
    w_fc2,
    weight_sem,
    halo,
    sum_send,
    sum_got,
    edge_send_sem,
    edge_recv_sem,
    sum_send_sem,
    sum_recv_sem,
    select_rows,
    fold,
    planes_wide,
    kernel_rows,
    residual,
    normed,
    outgoing,
    query_got,
    key_got,
    value_got,
    value_wide,
    mixed_send,
    mixed_got,
    attended,
    total,
    send_sem,
    recv_sem,
):
    me = lax.axis_index("ctx")
    planes, side, _ = density.shape
    tokens, width = residual.shape
    head_size = width // HEADS
    local_heads = max(HEADS // n, 1)
    groups = max(n // HEADS, 1)
    group_width = local_heads * head_size
    share = tokens // groups
    grid = side // STRIDE
    window = planes + 2

    weights = [
        pltpu.make_async_copy(source, target, weight_sem.at[i])
        for i, (source, target) in enumerate(
            ((w_qkv_hbm, w_qkv), (w_out_hbm, w_out), (w_fc1_hbm, w_fc1), (w_fc2_hbm, w_fc2))
        )
    ]
    for copy in weights:
        copy.start()

    barrier = pltpu.get_barrier_semaphore()

    def each_peer(action):
        def step(offset, carry):
            action(partner(me, n - offset, n))
            return carry

        lax.fori_loop(1, n, step, 0)

    each_peer(
        lambda peer: pl.semaphore_signal(
            barrier, inc=1, device_id={"ctx": peer}, device_id_type=MESH
        )
    )

    own = jnp.sum(density[...], axis=0)
    own = jnp.sum(own, axis=(0, 1), keepdims=True)
    sum_send[...] = jnp.broadcast_to(own, sum_send.shape)
    sum_got[me] = jnp.broadcast_to(own, sum_send.shape)

    @pl.when(me == 0)
    def _():
        halo[0] = jnp.ones((side, side), F32)

    @pl.when(me == n - 1)
    def _():
        halo[1] = jnp.ones((side, side), F32)

    pl.semaphore_wait(barrier, n - 1)

    def edge(side_index, plane, peer):
        return pltpu.make_async_remote_copy(
            src_ref=density.at[plane],
            dst_ref=halo.at[side_index],
            send_sem=edge_send_sem.at[side_index],
            recv_sem=edge_recv_sem.at[side_index],
            device_id={"ctx": peer},
            device_id_type=MESH,
        )

    up = edge(0, planes - 1, lax.rem(me + 1, n))
    down = edge(1, 0, lax.rem(me + n - 1, n))

    def sum_copy(source, peer):
        return pltpu.make_async_remote_copy(
            src_ref=sum_send,
            dst_ref=sum_got.at[source],
            send_sem=sum_send_sem.at[peer],
            recv_sem=sum_recv_sem.at[source],
            device_id={"ctx": peer},
            device_id_type=MESH,
        )

    each_peer(lambda peer: sum_copy(me, peer).start())

    @pl.when(me < n - 1)
    def _():
        up.start()

    @pl.when(me > 0)
    def _():
        down.start()

    pair = 2 * side
    row = iota((tokens, side), 0)
    col = iota((tokens, side), 1)
    for b in range(KERNEL):
        hit = col == STRIDE * (row // grid) - 1 + b
        select_rows[b] = jnp.where(hit, 1.0, 0.0).astype(BF16)
    lane_row = iota((pair, 256), 0)
    lane_col = iota((pair, 256), 1)
    high = lane_row // side
    offset_c = ((lane_row + 1) & (STRIDE - 1)) + STRIDE * high
    for b in range(KERNEL):
        for a in range(window):
            hit = (offset_c < KERNEL) & (lane_col == (a * KERNEL + b) * KERNEL + offset_c)
            fold[b, a * pair : (a + 1) * pair, :] = jnp.where(hit, 1.0, 0.0).astype(BF16)
    taps = stem_weight.shape[0]
    kernel_rows[...] = jnp.zeros(kernel_rows.shape, BF16)
    kernel_rows[0:taps, :] = stem_weight[...]
    tile_row = iota((tokens, pair), 0)
    tile_lane = iota((tokens, pair), 1)
    keep = (((tile_lane & (side - 1)) + 1) // STRIDE - tile_lane // side) == (
        tile_row & (grid - 1)
    )
    keep = jnp.where(keep, 1.0, 0.0).astype(BF16)

    each_peer(lambda peer: sum_copy(peer, peer).wait_recv())

    @pl.when(me > 0)
    def _():
        up.wait_recv()

    @pl.when(me < n - 1)
    def _():
        down.wait_recv()

    mean_density = (jnp.sum(sum_got[...], axis=0)[0:1, 0:1]) / cells
    for a in range(window):
        if a == 0:
            plane = jnp.where(me > 0, jnp.log(halo[0] / mean_density), 0.0)
        elif a == window - 1:
            plane = jnp.where(me < n - 1, jnp.log(halo[1] / mean_density), 0.0)
        else:
            plane = jnp.log(density[a - 1] / mean_density)
        plane = plane.astype(BF16)
        planes_wide[:, a * pair : (a + 1) * pair] = jnp.concatenate([plane, plane], axis=1)

    keep_wide = jnp.concatenate([keep] * window, axis=1)
    patches = jnp.zeros((tokens, 256), F32)
    for b in range(KERNEL):
        rows = jnp.dot(select_rows[b], planes_wide[...], preferred_element_type=F32)
        rows = rows.astype(BF16) * keep_wide
        patches += jnp.dot(rows, fold[b], preferred_element_type=F32)
    embedded = jnp.dot(patches.astype(BF16), kernel_rows[...], preferred_element_type=F32)
    embedded = embedded + stem_bias[...] + pos_embed[...].astype(F32)
    residual[...] = embedded.astype(BF16)
    normed[...] = norm_rows(residual[...].astype(F32), ln1_gain[...], ln1_bias[...]).astype(BF16)

    def head_group(peer):
        return peer // groups

    def my_rows(peer):
        return pl.ds(pl.multiple_of(lax.rem(peer, groups) * share, share), share)

    def projected_copy(kind, source, peer):
        piece = outgoing.at[kind, head_group(peer)]
        got = (query_got, key_got, value_got)[kind]
        if kind == 0:
            piece = piece.at[my_rows(peer)]
        return pltpu.make_async_remote_copy(
            src_ref=piece,
            dst_ref=got.at[source],
            send_sem=send_sem.at[kind, peer],
            recv_sem=recv_sem.at[kind, source],
            device_id={"ctx": peer},
            device_id_type=MESH,
        )

    weights[0].wait()
    block = 256
    for kind in (1, 2, 0):
        for start in range(0, width, block):
            columns = slice(kind * width + start, kind * width + start + block)
            result = jnp.dot(normed[...], w_qkv[:, columns], preferred_element_type=F32)
            result = result + qkv_bias[:, columns]
            if kind == 0:
                result = result * (1.0 / head_size**0.5)
            result = result.astype(BF16)
            for part in range(block // group_width):
                outgoing[kind, start // group_width + part] = result[
                    :, part * group_width : (part + 1) * group_width
                ]
        each_peer(lambda peer: projected_copy(kind, me, peer).start())
    query_got[me] = outgoing[0, head_group(me), my_rows(me), :]
    key_got[me] = outgoing[1, head_group(me)]
    value_got[me] = outgoing[2, head_group(me)]

    each_peer(lambda peer: projected_copy(1, peer, peer).wait_recv())
    each_peer(lambda peer: projected_copy(2, peer, peer).wait_recv())

    keys_total = n * tokens
    wide = group_width % 128 == 0
    if wide:
        value_wide[:, 0:group_width] = value_got[...].reshape(keys_total, group_width)
        value_wide[:, group_width:] = jnp.ones((keys_total, group_width), BF16)

    def mixed_copy(source, peer):
        return pltpu.make_async_remote_copy(
            src_ref=mixed_send.at[peer],
            dst_ref=mixed_got.at[source],
            send_sem=send_sem.at[3, peer],
            recv_sem=recv_sem.at[3, source],
            device_id={"ctx": peer},
            device_id_type=MESH,
        )

    def attend(offset, carry):
        peer = partner(me, lax.rem(n - offset, n), n)

        @pl.when(offset > 0)
        def _():
            projected_copy(0, peer, peer).wait_recv()

        rows = min(share, ROWS)
        for first in range(0, share, rows):
            query = query_got[peer, first : first + rows, :]
            lane = iota((rows, group_width), 1) // head_size
            mixed = None
            for head in range(local_heads):
                mine = query
                if local_heads > 1:
                    mine = jnp.where(lane == head, query, jnp.zeros_like(query))
                scores = lax.dot_general(
                    mine,
                    key_got[...].reshape(keys_total, group_width),
                    (((1,), (1,)), ((), ())),
                    preferred_element_type=F32,
                )
                weight = jnp.exp(scores - jnp.max(scores, axis=1, keepdims=True))
                values = value_wide[...] if wide else value_got[...].reshape(keys_total, group_width)
                product = jnp.dot(weight.astype(BF16), values, preferred_element_type=F32)
                if wide:
                    part = product[:, 0:group_width] / product[:, group_width:]
                else:
                    part = product / jnp.sum(weight, axis=1, keepdims=True)
                mixed = part if mixed is None else jnp.where(lane == head, part, mixed)
            mixed_send[peer, first : first + rows, :] = mixed.astype(BF16)

        @pl.when(offset > 0)
        def _():
            mixed_copy(me, peer).start()

        @pl.when(offset == 0)
        def _():
            mixed_got[me] = mixed_send[me]

        return carry

    lax.fori_loop(0, n, attend, 0)

    each_peer(lambda peer: mixed_copy(peer, peer).wait_recv())
    for piece in range(n):
        first = (piece % groups) * share
        column = (piece // groups) * group_width
        attended[first : first + share, column : column + group_width] = mixed_got[piece]

    weights[1].wait()
    stream = (
        residual[...].astype(F32)
        + jnp.dot(attended[...], w_out[...], preferred_element_type=F32)
        + out_bias[...]
    ).astype(BF16)
    residual[...] = stream
    stream = stream.astype(F32)
    normed[...] = norm_rows(stream, ln2_gain[...], ln2_bias[...]).astype(BF16)
    total[...] = stream + fc2_bias[...]

    weights[2].wait()
    weights[3].wait()
    hidden_width = w_fc1.shape[1]
    tile = math.gcd(hidden_width, 512)
    for start in range(0, hidden_width, tile):
        columns = slice(start, start + tile)
        hidden = jnp.dot(normed[...], w_fc1[:, columns], preferred_element_type=F32)
        hidden = hidden + fc1_bias[:, columns]
        hidden = 0.5 * hidden * (1.0 + lax.erf(hidden * math.sqrt(0.5)))
        total[...] += jnp.dot(hidden.astype(BF16), w_fc2[columns, :], preferred_element_type=F32)
    encoded[...] = total[...].astype(BF16)

    def finish(peer):
        sum_copy(me, peer).wait_send()
        for kind in range(3):
            projected_copy(kind, me, peer).wait_send()
        mixed_copy(me, peer).wait_send()

    each_peer(finish)

    @pl.when(me < n - 1)
    def _():
        up.wait_send()

    @pl.when(me > 0)
    def _():
        down.wait_send()


def stem_tables(side, features):
    grid = side // STRIDE
    tokens = grid * grid
    token = np.arange(tokens)
    select = np.zeros((STRIDE, tokens, side), np.float32)
    for b in range(STRIDE):
        select[b, token, STRIDE * (token // grid) + b] = 1
    x = np.arange(side)
    keep = np.tile(x[None, :] // STRIDE == token[:, None] % grid, (1, STRIDE))
    fold = np.zeros((STRIDE, STRIDE, side, 256), np.float32)
    for b in range(STRIDE):
        for a in range(STRIDE):
            lane = (a * STRIDE + b) * STRIDE + x % STRIDE
            fold[b, a, x, lane] = 1
            fold[b, a, x, 192 + lane] = 1
    expand = np.zeros((3, 3, 128, 256), np.float32)
    shifts = {0: 0, -1: 1, 1: 2}
    for a in range(KERNEL):
        for b in range(KERNEL):
            for c in range(KERNEL):
                block = ((a - 1) % STRIDE * STRIDE + (b - 1) % STRIDE) * STRIDE + (c - 1) % STRIDE
                lane = (a * KERNEL + b) * KERNEL + c
                expand[shifts[(b - 1) // STRIDE], shifts[(c - 1) // STRIDE], block, lane] = 1
    return [
        jnp.asarray(table.reshape(-1, table.shape[-1]), BF16)
        for table in (select, keep.astype(np.float32), fold, expand)
    ]


def shares_positions(n, replicas, density, pos_embed):
    planes, side, _ = density.shape
    tokens, width = pos_embed.shape
    return (
        replicas == 4
        and n % 2 == 0
        and n <= HEADS
        and (HEADS // n) * (width // HEADS) == 128
        and planes == STRIDE
        and side == 64
        and tokens == (side // STRIDE) ** 2
    )


def shared_kernel(
    n,
    cells,
    density,
    stem_weight,
    stem_bias,
    pos_embed,
    ln1_gain,
    ln1_bias,
    w_qkv_hbm,
    qkv_bias,
    w_out_hbm,
    out_bias,
    ln2_gain,
    ln2_bias,
    w_fc1_hbm,
    fc1_bias,
    w_fc2_hbm,
    fc2_bias,
    select_hbm,
    keep_hbm,
    fold_hbm,
    expand_hbm,
    encoded,
    w_qkv,
    w_out,
    w_fc1,
    w_fc2,
    select,
    keep,
    fold,
    expand,
    qkv_sem,
    weight_sem,
    table_sem,
    sum_send,
    sum_got,
    stats_send,
    stats_got,
    blocks_send,
    blocks,
    windows,
    kernel_raw,
    kernel_mixed,
    position,
    residual,
    normed,
    part_send,
    part,
    query,
    key,
    value_wide,
    mixed_send,
    mixed_got,
    attended,
    total,
    sum_send_sem,
    sum_recv_sem,
    stats_send_sem,
    stats_recv_sem,
    blocks_send_sem,
    blocks_recv_sem,
    part_send_sem,
    part_recv_sem,
    mixed_send_sem,
    mixed_recv_sem,
):
    me = lax.axis_index("ctx")
    replica = lax.axis_index("dp")
    near = replica + 1 - 2 * lax.rem(replica, 2)
    across = lax.rem(replica + 2, 4)
    diagonal = lax.rem(near + 2, 4)
    tokens, width = residual.shape
    side = density.shape[1]
    grid = side // STRIDE
    head_size = width // HEADS
    local_heads = HEADS // n
    lanes = 128
    share = tokens // 4
    pairs = n // 2
    my_pair, my_side = me // 2, lax.rem(me, 2)
    twin = 2 * my_pair + 1 - my_side

    def pair_at(step):
        return partner(my_pair, pairs - 1 - step, pairs)

    def qkv_copy(step, kind):
        start = pl.multiple_of(kind * width + pair_at(step) * 2 * lanes, 2 * lanes)
        return pltpu.make_async_copy(
            w_qkv_hbm.at[:, pl.ds(start, 2 * lanes)], w_qkv.at[step, kind], qkv_sem.at[step, kind]
        )

    tables = [
        pltpu.make_async_copy(source, target, table_sem.at[i])
        for i, (source, target) in enumerate(
            ((select_hbm, select), (keep_hbm, keep), (fold_hbm, fold), (expand_hbm, expand))
        )
    ]
    weights = [
        pltpu.make_async_copy(source, target, weight_sem.at[i])
        for i, (source, target) in enumerate(
            ((w_out_hbm, w_out), (w_fc1_hbm, w_fc1), (w_fc2_hbm, w_fc2))
        )
    ]
    for kind in range(3):
        qkv_copy(0, kind).start()
    for copy in tables:
        copy.start()
    for step in range(1, pairs):
        for kind in range(3):
            qkv_copy(step, kind).start()

    barrier = pltpu.get_barrier_semaphore()

    def each_peer(action):
        def step(offset, carry):
            action(partner(me, n - offset, n))
            return carry

        lax.fori_loop(1, n, step, 0)

    each_peer(
        lambda peer: pl.semaphore_signal(
            barrier, inc=1, device_id={"ctx": peer}, device_id_type=MESH
        )
    )
    for other in (near, across):
        pl.semaphore_signal(barrier, inc=1, device_id={"dp": other}, device_id_type=MESH)

    own = jnp.sum(density[...], axis=0)
    own = jnp.sum(own, axis=(0, 1), keepdims=True)
    sum_send[...] = jnp.broadcast_to(own, sum_send.shape)
    sum_got[me] = jnp.broadcast_to(own, sum_send.shape)
    pl.semaphore_wait(barrier, n + 1)

    def remote(source, target, send, recv, **device):
        return pltpu.make_async_remote_copy(
            src_ref=source,
            dst_ref=target,
            send_sem=send,
            recv_sem=recv,
            device_id=device,
            device_id_type=MESH,
        )

    def sum_copy(source, peer):
        return remote(
            sum_send, sum_got.at[source], sum_send_sem.at[peer], sum_recv_sem.at[source], ctx=peer
        )

    each_peer(lambda peer: sum_copy(me, peer).start())

    centred = pos_embed[...].astype(F32) + stem_bias[...]
    centred = centred - jnp.mean(centred, axis=1, keepdims=True)
    position[...] = (centred * ln1_gain[...]).astype(BF16)

    def rows_of(which):
        return pl.ds(pl.multiple_of(which * share, share), share)

    def part_copy(step, other):
        return remote(
            part_send.at[2 * step + other],
            part.at[me, rows_of(replica)],
            part_send_sem.at[0, 2 * step + other],
            part_recv_sem.at[0, me],
            ctx=2 * pair_at(step) + other,
        )

    def part_got(source):
        return remote(
            part_send.at[0],
            part.at[source, rows_of(replica)],
            part_send_sem.at[0, 0],
            part_recv_sem.at[0, source],
            ctx=source,
        )

    def relay(hop, source, owner, target):
        piece = part.at[source, rows_of(owner)]
        return remote(
            piece, piece, part_send_sem.at[hop, source], part_recv_sem.at[hop, source], dp=target
        )

    def project_positions(step):
        rows = position[rows_of(replica), :]
        for kind in range(3):
            qkv_copy(step, kind).wait()
            result = jnp.dot(rows, w_qkv[step, kind], preferred_element_type=F32).astype(BF16)
            for other in range(2):
                part_send[2 * step + other, :, kind * lanes : (kind + 1) * lanes] = result[
                    :, other * lanes : (other + 1) * lanes
                ]
        for other in range(2):
            if step < pairs - 1:
                part_copy(step, other).start()
            else:

                @pl.when(my_side != other)
                def _():
                    part_copy(step, other).start()

    project_positions(0)

    each_peer(lambda peer: sum_copy(peer, peer).wait_recv())
    mean_density = (jnp.sum(sum_got[...], axis=0)[0:1, 0:1]) / cells
    for copy in tables:
        copy.wait()
    planes = [jnp.log(density[a] / mean_density).astype(BF16) for a in range(STRIDE)]
    planes = jnp.concatenate(planes, axis=1)
    picked = jnp.dot(select[...], planes, preferred_element_type=F32).astype(BF16)
    picked = [picked[b * tokens : (b + 1) * tokens] * keep[...] for b in range(STRIDE)]
    folded = jnp.dot(jnp.concatenate(picked, axis=1), fold[...], preferred_element_type=F32)
    half = tokens // 2
    folded = folded[0:half, 0:lanes] + folded[half:, lanes:]
    blocks_send[...] = folded.astype(BF16)
    blocks[me] = folded.astype(BF16)

    def blocks_copy(slot, peer):
        return remote(
            blocks_send,
            blocks.at[me],
            blocks_send_sem.at[slot],
            blocks_recv_sem.at[me],
            ctx=peer,
        )

    def blocks_relay(source, slot):
        return remote(
            blocks.at[source],
            blocks.at[source],
            blocks_send_sem.at[slot],
            blocks_recv_sem.at[source],
            ctx=twin,
        )

    for step in range(pairs - 1):
        blocks_copy(step, 2 * pair_at(step) + my_side).start()
    blocks_copy(pairs - 1, twin).start()

    for step in range(1, pairs):
        project_positions(step)
    for copy in weights:
        copy.start()

    my_lanes = pl.ds(pl.multiple_of(my_side * lanes, lanes), lanes)
    mine = jnp.concatenate([w_qkv[pairs - 1, kind, :, my_lanes] for kind in range(3)], axis=1)
    part[me] = jnp.dot(position[...], mine, preferred_element_type=F32).astype(BF16)
    taps = stem_weight.shape[0]
    kernel_raw[...] = jnp.zeros(kernel_raw.shape, BF16)
    kernel_raw[0:taps, :] = stem_weight[...]
    kernel_mixed[...] = jnp.zeros(kernel_mixed.shape, BF16)
    kernel = stem_weight[...].astype(F32)
    kernel = (kernel - jnp.mean(kernel, axis=1, keepdims=True)) * ln1_gain[...]
    kernel_mixed[0:taps, :] = kernel.astype(BF16)
    high = ln1_bias[...].astype(BF16)
    low = (ln1_bias[...] - high.astype(F32)).astype(BF16)
    line = iota((8, width), 0)
    bias_rows = jnp.where(line == 0, high.astype(F32), jnp.where(line == 1, low.astype(F32), 0.0))
    kernel_mixed[taps : taps + 8, :] = bias_rows.astype(BF16)
    mixing = jnp.dot(kernel_mixed[...], mine, preferred_element_type=F32)
    shift = mixing[taps : taps + 1] + mixing[taps + 1 : taps + 2]
    my_bias = [
        qkv_bias[:, pl.ds(pl.multiple_of(kind * width + me * lanes, lanes), lanes)]
        for kind in range(3)
    ]
    shift = shift + jnp.concatenate(my_bias, axis=1)
    mixing = mixing.astype(BF16)

    def relay_first(step):
        for other in range(2):

            def pass_on():
                source = 2 * pair_at(step) + other
                part_got(source).wait_recv()
                relay(1, source, replica, near).start()
                relay(2, source, replica, across).start()

            if step < pairs - 1:
                pass_on()
            else:
                pl.when(my_side != other)(pass_on)

    def relay_second(step):
        for other in range(2):

            def pass_on():
                source = 2 * pair_at(step) + other
                relay(2, source, across, across).wait_recv()
                relay(3, source, across, near).start()

            if step < pairs - 1:
                pass_on()
            else:
                pl.when(my_side != other)(pass_on)

    relay_first(0)
    for step in range(pairs - 1):
        source = 2 * pair_at(step) + my_side
        blocks_relay(source, 0).wait_recv()
        blocks_relay(source, pairs + step).start()
    relay_first(1)
    for step in range(pairs):
        source = 2 * pair_at(step) + 1 - my_side
        blocks_relay(source, 0).wait_recv()

    for t in range(n):
        packed = blocks[t].astype(F32)
        spread = jnp.concatenate([packed, pltpu.roll(packed, lanes // 2, 1)], axis=0)
        column = iota(spread.shape, 0) & (grid - 1)
        before = jnp.where(column == 0, 0.0, pltpu.roll(spread, 1, 0))
        after = jnp.where(column == grid - 1, 0.0, pltpu.roll(spread, tokens - 1, 0))
        wide = jnp.concatenate([v.astype(BF16) for v in (spread, before, after)], axis=1)
        edge = jnp.zeros((grid, wide.shape[1]), BF16)
        above = jnp.concatenate([edge, wide[: tokens - grid]], axis=0)
        below = jnp.concatenate([wide[grid:], edge], axis=0)
        wide = jnp.concatenate([wide, above, below], axis=1)
        windows[t] = jnp.dot(wide, expand[...], preferred_element_type=F32).astype(BF16)

    tap = iota((tokens, 256), 1)
    face = KERNEL * KERNEL

    def patches_of(before, here, after):
        inner = jnp.where(tap < taps - face, here, after)
        return jnp.where(tap < face, before, inner)

    before = windows[lax.rem(me + n - 1, n)]
    after = windows[lax.rem(me + 1, n)]
    before = jnp.where(me > 0, before, jnp.zeros_like(before))
    after = jnp.where(me < n - 1, after, jnp.zeros_like(after))
    patches = patches_of(before, windows[me], after)
    embedded = jnp.dot(patches, kernel_raw[...], preferred_element_type=F32)
    embedded = embedded + stem_bias[...] + pos_embed[...].astype(F32)
    residual[...] = embedded.astype(BF16)
    centre = residual[...].astype(F32)
    centre = centre - jnp.mean(centre, axis=1, keepdims=True)
    inverse = lax.rsqrt(jnp.mean(centre * centre, axis=1, keepdims=True) + 1e-06)
    inverse = jnp.broadcast_to(inverse, (tokens, lanes))
    stats = [inverse[i * lanes : (i + 1) * lanes].T[0:1] for i in range(tokens // lanes)]
    stats.append(jnp.zeros((8 - len(stats), lanes), F32))
    stats = jnp.concatenate(stats, axis=0)
    stats_send[...] = stats
    stats_got[me] = stats

    def stats_copy(source, peer):
        return remote(
            stats_send,
            stats_got.at[source],
            stats_send_sem.at[peer],
            stats_recv_sem.at[source],
            ctx=peer,
        )

    each_peer(lambda peer: stats_copy(me, peer).start())

    relay_second(0)
    for step in range(2, pairs):
        relay_first(step)
        relay_second(step - 1)
    relay_second(pairs - 1)

    each_peer(lambda peer: stats_copy(peer, peer).wait_recv())

    def arrived(source):
        relay(1, source, near, near).wait_recv()
        relay(3, source, diagonal, near).wait_recv()

    each_peer(arrived)

    scales = (1.0 / head_size**0.5, 1.0, 1.0)
    for t in range(n):
        nothing = jnp.zeros((tokens, 256), BF16)
        patches = patches_of(
            windows[t - 1] if t > 0 else nothing,
            windows[t],
            windows[t + 1] if t < n - 1 else nothing,
        )
        result = jnp.dot(patches, mixing, preferred_element_type=F32) + part[t].astype(F32)
        inverse = jnp.concatenate(
            [
                jnp.broadcast_to(stats_got[t, i : i + 1, :], (lanes, lanes)).T
                for i in range(tokens // lanes)
            ],
            axis=0,
        )
        for kind, scale in enumerate(scales):
            columns = slice(kind * lanes, (kind + 1) * lanes)
            rows = result[:, columns] * inverse + shift[:, columns]
            if kind == 0:
                query[t] = (rows * scale).astype(BF16)
            elif kind == 1:
                key[t] = rows.astype(BF16)
            else:
                value_wide[t * tokens : (t + 1) * tokens, 0:lanes] = rows.astype(BF16)
    keys_total = n * tokens
    value_wide[:, lanes:] = jnp.ones((keys_total, lanes), BF16)

    def mixed_copy(source, peer):
        return remote(
            mixed_send.at[peer],
            mixed_got.at[source],
            mixed_send_sem.at[peer],
            mixed_recv_sem.at[source],
            ctx=peer,
        )

    def attend(offset, carry):
        peer = partner(me, n - 1 - offset, n)
        rows = min(tokens, ROWS)
        for first in range(0, tokens, rows):
            picked = query[peer, first : first + rows, :]
            lane = iota((rows, lanes), 1) // head_size
            mixed = None
            for head in range(local_heads):
                mine = jnp.where(lane == head, picked, jnp.zeros_like(picked))
                scores = lax.dot_general(
                    mine,
                    key[...].reshape(keys_total, lanes),
                    (((1,), (1,)), ((), ())),
                    preferred_element_type=F32,
                )
                weight = jnp.exp(scores - jnp.max(scores, axis=1, keepdims=True))
                product = jnp.dot(
                    weight.astype(BF16), value_wide[...], preferred_element_type=F32
                )
                rows_mixed = product[:, 0:lanes] / product[:, lanes:]
                mixed = rows_mixed if mixed is None else jnp.where(lane == head, rows_mixed, mixed)
            mixed_send[peer, first : first + rows, :] = mixed.astype(BF16)

        @pl.when(offset < n - 1)
        def _():
            mixed_copy(me, peer).start()

        return carry

    lax.fori_loop(0, n, attend, 0)
    mixed_got[me] = mixed_send[me]

    each_peer(lambda peer: mixed_copy(peer, peer).wait_recv())
    for piece in range(n):
        attended[:, piece * lanes : (piece + 1) * lanes] = mixed_got[piece]

    weights[0].wait()
    stream = (
        residual[...].astype(F32)
        + jnp.dot(attended[...], w_out[...], preferred_element_type=F32)
        + out_bias[...]
    ).astype(BF16)
    stream = stream.astype(F32)
    normed[...] = norm_rows(stream, ln2_gain[...], ln2_bias[...]).astype(BF16)
    total[...] = stream + fc2_bias[...]

    weights[1].wait()
    weights[2].wait()
    hidden_width = w_fc1.shape[1]
    tile = math.gcd(hidden_width, 512)
    for start in range(0, hidden_width, tile):
        columns = slice(start, start + tile)
        hidden = jnp.dot(normed[...], w_fc1[:, columns], preferred_element_type=F32)
        hidden = hidden + fc1_bias[:, columns]
        hidden = 0.5 * hidden * (1.0 + lax.erf(hidden * math.sqrt(0.5)))
        total[...] += jnp.dot(hidden.astype(BF16), w_fc2[columns, :], preferred_element_type=F32)
    encoded[...] = total[...].astype(BF16)

    def finish(peer):
        sum_copy(me, peer).wait_send()
        stats_copy(me, peer).wait_send()
        mixed_copy(me, peer).wait_send()
        relay(1, peer, replica, near).wait_send()
        relay(2, peer, replica, across).wait_send()
        relay(3, peer, across, near).wait_send()

    each_peer(finish)
    for step in range(pairs - 1):
        for other in range(2):
            part_copy(step, other).wait_send()
        blocks_copy(step, 2 * pair_at(step) + my_side).wait_send()
        blocks_relay(2 * pair_at(step) + my_side, pairs + step).wait_send()
    for other in range(2):

        @pl.when(my_side != other)
        def _():
            part_copy(pairs - 1, other).wait_send()

    blocks_copy(pairs - 1, twin).wait_send()


def shared_call(
    density,
    stem_weight,
    stem_bias,
    pos_embed,
    ln1_gain,
    ln1_bias,
    w_qkv,
    qkv_bias,
    w_out,
    out_bias,
    ln2_gain,
    ln2_bias,
    w_fc1,
    fc1_bias,
    w_fc2,
    fc2_bias,
):
    n = lax.axis_size("ctx")
    tokens, width = pos_embed.shape
    side = density.shape[1]
    vmem = pl.BlockSpec(memory_space=pltpu.VMEM)
    hbm = pl.BlockSpec(memory_space=pl.ANY)
    tables = stem_tables(side, stem_weight.shape[0])

    def line(vector):
        return vector.reshape(1, -1)

    dma = pltpu.SemaphoreType.DMA
    lanes = 128
    pairs = n // 2
    return pl.pallas_call(
        functools.partial(shared_kernel, n, density.size * n),
        out_shape=jax.ShapeDtypeStruct((tokens, width), BF16),
        in_specs=[
            vmem, vmem, vmem, vmem, vmem, vmem, hbm, vmem,
            hbm, vmem, vmem, vmem, hbm, vmem, hbm, vmem,
            hbm, hbm, hbm, hbm,
        ],
        out_specs=vmem,
        scratch_shapes=[
            pltpu.VMEM((pairs, 3, width, 2 * lanes), BF16),
            pltpu.VMEM(w_out.shape, BF16),
            pltpu.VMEM(w_fc1.shape, BF16),
            pltpu.VMEM(w_fc2.shape, BF16),
            *[pltpu.VMEM(table.shape, BF16) for table in tables],
            dma((pairs, 3)),
            dma((3,)),
            dma((4,)),
            pltpu.VMEM((8, lanes), F32),
            pltpu.VMEM((n, 8, lanes), F32),
            pltpu.VMEM((8, lanes), F32),
            pltpu.VMEM((n, 8, lanes), F32),
            pltpu.VMEM((tokens // 2, lanes), BF16),
            pltpu.VMEM((n, tokens // 2, lanes), BF16),
            pltpu.VMEM((n, tokens, 256), BF16),
            pltpu.VMEM((256, width), BF16),
            pltpu.VMEM((256, width), BF16),
            pltpu.VMEM((tokens, width), BF16),
            pltpu.VMEM((tokens, width), BF16),
            pltpu.VMEM((tokens, width), BF16),
            pltpu.VMEM((n, tokens // 4, 3 * lanes), BF16),
            pltpu.VMEM((n, tokens, 3 * lanes), BF16),
            pltpu.VMEM((n, tokens, lanes), BF16),
            pltpu.VMEM((n, tokens, lanes), BF16),
            pltpu.VMEM((n * tokens, 2 * lanes), BF16),
            pltpu.VMEM((n, tokens, lanes), BF16),
            pltpu.VMEM((n, tokens, lanes), BF16),
            pltpu.VMEM((tokens, width), BF16),
            pltpu.VMEM((tokens, width), F32),
            dma((n,)),
            dma((n,)),
            dma((n,)),
            dma((n,)),
            dma((2 * pairs,)),
            dma((n,)),
            dma((4, n)),
            dma((4, n)),
            dma((n,)),
            dma((n,)),
        ],
        compiler_params=pltpu.CompilerParams(
            collective_id=1, has_side_effects=True, vmem_limit_bytes=60 * 1024 * 1024
        ),
    )(
        density,
        stem_weight,
        line(stem_bias),
        pos_embed,
        line(ln1_gain),
        line(ln1_bias),
        w_qkv,
        line(qkv_bias),
        w_out,
        line(out_bias),
        line(ln2_gain),
        line(ln2_bias),
        w_fc1,
        line(fc1_bias),
        w_fc2,
        line(fc2_bias),
        *tables,
    )


def per_device(
    density,
    stem_weight,
    stem_bias,
    pos_embed,
    ln1_gain,
    ln1_bias,
    w_qkv,
    qkv_bias,
    w_out,
    out_bias,
    ln2_gain,
    ln2_bias,
    w_fc1,
    fc1_bias,
    w_fc2,
    fc2_bias,
):
    n = lax.axis_size("ctx")
    tokens, width = pos_embed.shape
    if shares_positions(n, lax.axis_size("dp"), density, pos_embed):
        return shared_call(
            density, stem_weight, stem_bias, pos_embed, ln1_gain, ln1_bias, w_qkv, qkv_bias,
            w_out, out_bias, ln2_gain, ln2_bias, w_fc1, fc1_bias, w_fc2, fc2_bias,
        )
    hidden_width = w_fc1.shape[1]
    planes, side, _ = density.shape
    assert planes == STRIDE and tokens == (side // STRIDE) ** 2
    head_size = width // HEADS
    local_heads = max(HEADS // n, 1)
    groups = max(n // HEADS, 1)
    head_groups = HEADS // local_heads
    group_width = local_heads * head_size
    share = tokens // groups
    pair = 2 * side
    window = planes + 2
    vmem = pl.BlockSpec(memory_space=pltpu.VMEM)
    hbm = pl.BlockSpec(memory_space=pl.ANY)

    def line(vector):
        return vector.reshape(1, -1)

    dma = pltpu.SemaphoreType.DMA
    wide_shape = (n * tokens, 2 * group_width) if group_width % 128 == 0 else (16, 128)
    return pl.pallas_call(
        functools.partial(layer_kernel, n, density.size * n),
        out_shape=jax.ShapeDtypeStruct((tokens, width), BF16),
        in_specs=[
            vmem, vmem, vmem, vmem, vmem, vmem, hbm, vmem,
            hbm, vmem, vmem, vmem, hbm, vmem, hbm, vmem,
        ],
        out_specs=vmem,
        scratch_shapes=[
            pltpu.VMEM(w_qkv.shape, BF16),
            pltpu.VMEM(w_out.shape, BF16),
            pltpu.VMEM(w_fc1.shape, BF16),
            pltpu.VMEM(w_fc2.shape, BF16),
            dma((4,)),
            pltpu.VMEM((2, side, side), F32),
            pltpu.VMEM((8, 128), F32),
            pltpu.VMEM((n, 8, 128), F32),
            dma((2,)),
            dma((2,)),
            dma((n,)),
            dma((n,)),
            pltpu.VMEM((KERNEL, tokens, side), BF16),
            pltpu.VMEM((KERNEL, window * pair, 256), BF16),
            pltpu.VMEM((side, window * pair), BF16),
            pltpu.VMEM((256, width), BF16),
            pltpu.VMEM((tokens, width), BF16),
            pltpu.VMEM((tokens, width), BF16),
            pltpu.VMEM((3, head_groups, tokens, group_width), BF16),
            pltpu.VMEM((n, share, group_width), BF16),
            pltpu.VMEM((n, tokens, group_width), BF16),
            pltpu.VMEM((n, tokens, group_width), BF16),
            pltpu.VMEM(wide_shape, BF16),
            pltpu.VMEM((n, share, group_width), BF16),
            pltpu.VMEM((n, share, group_width), BF16),
            pltpu.VMEM((tokens, width), BF16),
            pltpu.VMEM((tokens, width), F32),
            dma((4, n)),
            dma((4, n)),
        ],
        compiler_params=pltpu.CompilerParams(
            collective_id=0, has_side_effects=True, vmem_limit_bytes=60 * 1024 * 1024
        ),
    )(
        density,
        stem_weight,
        line(stem_bias),
        pos_embed,
        line(ln1_gain),
        line(ln1_bias),
        w_qkv,
        line(qkv_bias),
        w_out,
        line(out_bias),
        line(ln2_gain),
        line(ln2_bias),
        w_fc1,
        line(fc1_bias),
        w_fc2,
        line(fc2_bias),
    )


def solution(mesh):
    in_specs = (P(("dp", "ctx"), None, None), P(), P(), P("ctx", None)) + (P(),) * 12
    return jax.shard_map(
        per_device,
        mesh=mesh,
        in_specs=in_specs,
        out_specs=P(("dp", "ctx"), None),
        check_vma=False,
    )
```

```python
import functools
import math

import jax
import jax.numpy as jnp
import numpy as np
from jax import lax
from jax.experimental import pallas as pl
from jax.experimental.pallas import tpu as pltpu
from jax.sharding import PartitionSpec as P

HEADS = 16
KERNEL = 6
STRIDE = 4
ROWS = 128
MESH = pl.DeviceIdType.MESH
F32 = jnp.float32
BF16 = jnp.bfloat16


def iota(shape, axis):
    return lax.broadcasted_iota(jnp.int32, shape, axis)


def partner(me, mask, n):
    result, bit = 0, 1
    while bit < n:
        result += ((me // bit + mask // bit) % 2) * bit
        bit *= 2
    return result


def norm_rows(values, gain_vector, shift_vector):
    center = values - jnp.mean(values, axis=-1, keepdims=True)
    spread = jnp.mean(center * center, axis=-1, keepdims=True)
    return center * lax.rsqrt(spread + 1e-06) * gain_vector + shift_vector


def layer_kernel(
    n,
    cells,
    density,
    stem_weight,
    stem_bias,
    pos_embed,
    ln1_gain,
    ln1_bias,
    w_qkv_hbm,
    qkv_bias,
    w_out_hbm,
    out_bias,
    ln2_gain,
    ln2_bias,
    w_fc1_hbm,
    fc1_bias,
    w_fc2_hbm,
    fc2_bias,
    encoded,
    w_qkv,
    w_out,
    w_fc1,
    w_fc2,
    weight_sem,
    halo,
    sum_send,
    sum_got,
    edge_send_sem,
    edge_recv_sem,
    sum_send_sem,
    sum_recv_sem,
    select_rows,
    fold,
    planes_wide,
    kernel_rows,
    residual,
    normed,
    outgoing,
    query_got,
    key_got,
    value_got,
    value_wide,
    mixed_send,
    mixed_got,
    attended,
    total,
    send_sem,
    recv_sem,
):
    me = lax.axis_index("ctx")
    planes, side, _ = density.shape
    tokens, width = residual.shape
    head_size = width // HEADS
    local_heads = max(HEADS // n, 1)
    groups = max(n // HEADS, 1)
    group_width = local_heads * head_size
    share = tokens // groups
    grid = side // STRIDE
    window = planes + 2

    weights = [
        pltpu.make_async_copy(source, target, weight_sem.at[i])
        for i, (source, target) in enumerate(
            ((w_qkv_hbm, w_qkv), (w_out_hbm, w_out), (w_fc1_hbm, w_fc1), (w_fc2_hbm, w_fc2))
        )
    ]
    for copy in weights:
        copy.start()

    barrier = pltpu.get_barrier_semaphore()

    def each_peer(action):
        def step(offset, carry):
            action(partner(me, n - offset, n))
            return carry

        lax.fori_loop(1, n, step, 0)

    each_peer(
        lambda peer: pl.semaphore_signal(
            barrier, inc=1, device_id={"ctx": peer}, device_id_type=MESH
        )
    )

    own = jnp.sum(density[...], axis=0)
    own = jnp.sum(own, axis=(0, 1), keepdims=True)
    sum_send[...] = jnp.broadcast_to(own, sum_send.shape)
    sum_got[me] = jnp.broadcast_to(own, sum_send.shape)

    @pl.when(me == 0)
    def _():
        halo[0] = jnp.ones((side, side), F32)

    @pl.when(me == n - 1)
    def _():
        halo[1] = jnp.ones((side, side), F32)

    pl.semaphore_wait(barrier, n - 1)

    def edge(side_index, plane, peer):
        return pltpu.make_async_remote_copy(
            src_ref=density.at[plane],
            dst_ref=halo.at[side_index],
            send_sem=edge_send_sem.at[side_index],
            recv_sem=edge_recv_sem.at[side_index],
            device_id={"ctx": peer},
            device_id_type=MESH,
        )

    up = edge(0, planes - 1, lax.rem(me + 1, n))
    down = edge(1, 0, lax.rem(me + n - 1, n))

    def sum_copy(source, peer):
        return pltpu.make_async_remote_copy(
            src_ref=sum_send,
            dst_ref=sum_got.at[source],
            send_sem=sum_send_sem.at[peer],
            recv_sem=sum_recv_sem.at[source],
            device_id={"ctx": peer},
            device_id_type=MESH,
        )

    each_peer(lambda peer: sum_copy(me, peer).start())

    @pl.when(me < n - 1)
    def _():
        up.start()

    @pl.when(me > 0)
    def _():
        down.start()

    pair = 2 * side
    row = iota((tokens, side), 0)
    col = iota((tokens, side), 1)
    for b in range(KERNEL):
        hit = col == STRIDE * (row // grid) - 1 + b
        select_rows[b] = jnp.where(hit, 1.0, 0.0).astype(BF16)
    lane_row = iota((pair, 256), 0)
    lane_col = iota((pair, 256), 1)
    high = lane_row // side
    offset_c = ((lane_row + 1) & (STRIDE - 1)) + STRIDE * high
    for b in range(KERNEL):
        for a in range(window):
            hit = (offset_c < KERNEL) & (lane_col == (a * KERNEL + b) * KERNEL + offset_c)
            fold[b, a * pair : (a + 1) * pair, :] = jnp.where(hit, 1.0, 0.0).astype(BF16)
    taps = stem_weight.shape[0]
    kernel_rows[...] = jnp.zeros(kernel_rows.shape, BF16)
    kernel_rows[0:taps, :] = stem_weight[...]
    tile_row = iota((tokens, pair), 0)
    tile_lane = iota((tokens, pair), 1)
    keep = (((tile_lane & (side - 1)) + 1) // STRIDE - tile_lane // side) == (
        tile_row & (grid - 1)
    )
    keep = jnp.where(keep, 1.0, 0.0).astype(BF16)

    each_peer(lambda peer: sum_copy(peer, peer).wait_recv())

    @pl.when(me > 0)
    def _():
        up.wait_recv()

    @pl.when(me < n - 1)
    def _():
        down.wait_recv()

    mean_density = (jnp.sum(sum_got[...], axis=0)[0:1, 0:1]) / cells
    for a in range(window):
        if a == 0:
            plane = jnp.where(me > 0, jnp.log(halo[0] / mean_density), 0.0)
        elif a == window - 1:
            plane = jnp.where(me < n - 1, jnp.log(halo[1] / mean_density), 0.0)
        else:
            plane = jnp.log(density[a - 1] / mean_density)
        plane = plane.astype(BF16)
        planes_wide[:, a * pair : (a + 1) * pair] = jnp.concatenate([plane, plane], axis=1)

    keep_wide = jnp.concatenate([keep] * window, axis=1)
    patches = jnp.zeros((tokens, 256), F32)
    for b in range(KERNEL):
        rows = jnp.dot(select_rows[b], planes_wide[...], preferred_element_type=F32)
        rows = rows.astype(BF16) * keep_wide
        patches += jnp.dot(rows, fold[b], preferred_element_type=F32)
    embedded = jnp.dot(patches.astype(BF16), kernel_rows[...], preferred_element_type=F32)
    embedded = embedded + stem_bias[...] + pos_embed[...].astype(F32)
    residual[...] = embedded.astype(BF16)
    normed[...] = norm_rows(residual[...].astype(F32), ln1_gain[...], ln1_bias[...]).astype(BF16)

    def head_group(peer):
        return peer // groups

    def my_rows(peer):
        return pl.ds(pl.multiple_of(lax.rem(peer, groups) * share, share), share)

    def projected_copy(kind, source, peer):
        piece = outgoing.at[kind, head_group(peer)]
        got = (query_got, key_got, value_got)[kind]
        if kind == 0:
            piece = piece.at[my_rows(peer)]
        return pltpu.make_async_remote_copy(
            src_ref=piece,
            dst_ref=got.at[source],
            send_sem=send_sem.at[kind, peer],
            recv_sem=recv_sem.at[kind, source],
            device_id={"ctx": peer},
            device_id_type=MESH,
        )

    weights[0].wait()
    block = 256
    for kind in (1, 2, 0):
        for start in range(0, width, block):
            columns = slice(kind * width + start, kind * width + start + block)
            result = jnp.dot(normed[...], w_qkv[:, columns], preferred_element_type=F32)
            result = result + qkv_bias[:, columns]
            if kind == 0:
                result = result * (1.0 / head_size**0.5)
            result = result.astype(BF16)
            for part in range(block // group_width):
                outgoing[kind, start // group_width + part] = result[
                    :, part * group_width : (part + 1) * group_width
                ]
        each_peer(lambda peer: projected_copy(kind, me, peer).start())
    query_got[me] = outgoing[0, head_group(me), my_rows(me), :]
    key_got[me] = outgoing[1, head_group(me)]
    value_got[me] = outgoing[2, head_group(me)]

    each_peer(lambda peer: projected_copy(1, peer, peer).wait_recv())
    each_peer(lambda peer: projected_copy(2, peer, peer).wait_recv())

    keys_total = n * tokens
    wide = group_width % 128 == 0
    if wide:
        value_wide[:, 0:group_width] = value_got[...].reshape(keys_total, group_width)
        value_wide[:, group_width:] = jnp.ones((keys_total, group_width), BF16)

    def mixed_copy(source, peer):
        return pltpu.make_async_remote_copy(
            src_ref=mixed_send.at[peer],
            dst_ref=mixed_got.at[source],
            send_sem=send_sem.at[3, peer],
            recv_sem=recv_sem.at[3, source],
            device_id={"ctx": peer},
            device_id_type=MESH,
        )

    def attend(offset, carry):
        peer = partner(me, lax.rem(n - offset, n), n)

        @pl.when(offset > 0)
        def _():
            projected_copy(0, peer, peer).wait_recv()

        rows = min(share, ROWS)
        for first in range(0, share, rows):
            query = query_got[peer, first : first + rows, :]
            lane = iota((rows, group_width), 1) // head_size
            mixed = None
            for head in range(local_heads):
                mine = query
                if local_heads > 1:
                    mine = jnp.where(lane == head, query, jnp.zeros_like(query))
                scores = lax.dot_general(
                    mine,
                    key_got[...].reshape(keys_total, group_width),
                    (((1,), (1,)), ((), ())),
                    preferred_element_type=F32,
                )
                weight = jnp.exp(scores - jnp.max(scores, axis=1, keepdims=True))
                values = value_wide[...] if wide else value_got[...].reshape(keys_total, group_width)
                product = jnp.dot(weight.astype(BF16), values, preferred_element_type=F32)
                if wide:
                    part = product[:, 0:group_width] / product[:, group_width:]
                else:
                    part = product / jnp.sum(weight, axis=1, keepdims=True)
                mixed = part if mixed is None else jnp.where(lane == head, part, mixed)
            mixed_send[peer, first : first + rows, :] = mixed.astype(BF16)

        @pl.when(offset > 0)
        def _():
            mixed_copy(me, peer).start()

        @pl.when(offset == 0)
        def _():
            mixed_got[me] = mixed_send[me]

        return carry

    lax.fori_loop(0, n, attend, 0)

    each_peer(lambda peer: mixed_copy(peer, peer).wait_recv())
    for piece in range(n):
        first = (piece % groups) * share
        column = (piece // groups) * group_width
        attended[first : first + share, column : column + group_width] = mixed_got[piece]

    weights[1].wait()
    stream = (
        residual[...].astype(F32)
        + jnp.dot(attended[...], w_out[...], preferred_element_type=F32)
        + out_bias[...]
    ).astype(BF16)
    residual[...] = stream
    stream = stream.astype(F32)
    normed[...] = norm_rows(stream, ln2_gain[...], ln2_bias[...]).astype(BF16)
    total[...] = stream + fc2_bias[...]

    weights[2].wait()
    weights[3].wait()
    hidden_width = w_fc1.shape[1]
    tile = math.gcd(hidden_width, 512)
    for start in range(0, hidden_width, tile):
        columns = slice(start, start + tile)
        hidden = jnp.dot(normed[...], w_fc1[:, columns], preferred_element_type=F32)
        hidden = hidden + fc1_bias[:, columns]
        hidden = 0.5 * hidden * (1.0 + lax.erf(hidden * math.sqrt(0.5)))
        total[...] += jnp.dot(hidden.astype(BF16), w_fc2[columns, :], preferred_element_type=F32)
    encoded[...] = total[...].astype(BF16)

    def finish(peer):
        sum_copy(me, peer).wait_send()
        for kind in range(3):
            projected_copy(kind, me, peer).wait_send()
        mixed_copy(me, peer).wait_send()

    each_peer(finish)

    @pl.when(me < n - 1)
    def _():
        up.wait_send()

    @pl.when(me > 0)
    def _():
        down.wait_send()


def stem_tables(side, features):
    grid = side // STRIDE
    tokens = grid * grid
    token = np.arange(tokens)
    select = np.zeros((STRIDE, tokens, side), np.float32)
    for b in range(STRIDE):
        select[b, token, STRIDE * (token // grid) + b] = 1
    x = np.arange(side)
    keep = np.tile(x[None, :] // STRIDE == token[:, None] % grid, (1, STRIDE))
    fold = np.zeros((STRIDE, STRIDE, side, 256), np.float32)
    for b in range(STRIDE):
        for a in range(STRIDE):
            lane = (a * STRIDE + b) * STRIDE + x % STRIDE
            fold[b, a, x, lane] = 1
            fold[b, a, x, 192 + lane] = 1
    expand = np.zeros((3, 3, 128, 256), np.float32)
    shifts = {0: 0, -1: 1, 1: 2}
    for a in range(KERNEL):
        for b in range(KERNEL):
            for c in range(KERNEL):
                block = ((a - 1) % STRIDE * STRIDE + (b - 1) % STRIDE) * STRIDE + (c - 1) % STRIDE
                lane = (a * KERNEL + b) * KERNEL + c
                expand[shifts[(b - 1) // STRIDE], shifts[(c - 1) // STRIDE], block, lane] = 1
    return [
        jnp.asarray(table.reshape(-1, table.shape[-1]), BF16)
        for table in (select, keep.astype(np.float32), fold, expand)
    ]


def shares_positions(n, replicas, density, pos_embed):
    planes, side, _ = density.shape
    tokens, width = pos_embed.shape
    return (
        replicas == 4
        and n % 2 == 0
        and n <= HEADS
        and (HEADS // n) * (width // HEADS) == 128
        and planes == STRIDE
        and side == 64
        and tokens == (side // STRIDE) ** 2
    )


def shared_kernel(
    n,
    cells,
    density,
    stem_weight,
    stem_bias,
    pos_embed,
    ln1_gain,
    ln1_bias,
    w_qkv_hbm,
    qkv_bias,
    w_out_hbm,
    out_bias,
    ln2_gain,
    ln2_bias,
    w_fc1_hbm,
    fc1_bias,
    w_fc2_hbm,
    fc2_bias,
    select_hbm,
    keep_hbm,
    fold_hbm,
    expand_hbm,
    encoded,
    w_qkv,
    w_out,
    w_fc1,
    w_fc2,
    select,
    keep,
    fold,
    expand,
    qkv_sem,
    weight_sem,
    table_sem,
    sum_send,
    sum_got,
    stats_send,
    stats_got,
    blocks_send,
    blocks,
    windows,
    kernel_raw,
    kernel_mixed,
    position,
    residual,
    normed,
    part_send,
    part,
    query,
    key,
    value_wide,
    mixed_send,
    mixed_got,
    total,
    sum_send_sem,
    sum_recv_sem,
    stats_send_sem,
    stats_recv_sem,
    blocks_send_sem,
    blocks_recv_sem,
    part_send_sem,
    part_recv_sem,
    mixed_send_sem,
    mixed_recv_sem,
):
    me = lax.axis_index("ctx")
    replica = lax.axis_index("dp")
    near = replica + 1 - 2 * lax.rem(replica, 2)
    across = lax.rem(replica + 2, 4)
    diagonal = lax.rem(near + 2, 4)
    tokens, width = residual.shape
    side = density.shape[1]
    grid = side // STRIDE
    head_size = width // HEADS
    local_heads = HEADS // n
    lanes = 128
    share = tokens // 4
    pairs = n // 2
    my_pair, my_side = me // 2, lax.rem(me, 2)
    twin = 2 * my_pair + 1 - my_side

    def pair_at(step):
        return partner(my_pair, pairs - 1 - step, pairs)

    depth = width // 4

    def qkv_copy(piece):
        rows = pl.ds(piece * depth, depth)
        return pltpu.make_async_copy(w_qkv_hbm.at[rows], w_qkv.at[rows], qkv_sem.at[piece])

    tables = [
        pltpu.make_async_copy(source, target, table_sem.at[i])
        for i, (source, target) in enumerate(
            ((select_hbm, select), (keep_hbm, keep), (fold_hbm, fold), (expand_hbm, expand))
        )
    ]
    weights = [
        pltpu.make_async_copy(source, target, weight_sem.at[i])
        for i, (source, target) in enumerate(
            ((w_out_hbm, w_out), (w_fc1_hbm, w_fc1), (w_fc2_hbm, w_fc2))
        )
    ]
    for copy in tables:
        copy.start()
    for piece in range(4):
        qkv_copy(piece).start()

    barrier = pltpu.get_barrier_semaphore()

    def each_peer(action):
        def step(offset, carry):
            action(partner(me, n - offset, n))
            return carry

        lax.fori_loop(1, n, step, 0)

    each_peer(
        lambda peer: pl.semaphore_signal(
            barrier, inc=1, device_id={"ctx": peer}, device_id_type=MESH
        )
    )
    for other in (near, across):
        pl.semaphore_signal(barrier, inc=1, device_id={"dp": other}, device_id_type=MESH)

    def everywhere(values):
        return jnp.sum(jnp.sum(values, axis=0), axis=(0, 1), keepdims=True)

    logs = jnp.log(density[...])
    level = everywhere(logs) / (density.shape[0] * side * side)
    line = iota(sum_send.shape, 0)
    own = jnp.where(line == 0, everywhere(density[...]), level)
    sum_send[...] = own
    sum_got[me] = own
    def remote(source, target, send, recv, **device):
        return pltpu.make_async_remote_copy(
            src_ref=source,
            dst_ref=target,
            send_sem=send,
            recv_sem=recv,
            device_id=device,
            device_id_type=MESH,
        )

    def sum_copy(source, peer):
        return remote(
            sum_send, sum_got.at[source], sum_send_sem.at[peer], sum_recv_sem.at[source], ctx=peer
        )


    centred = pos_embed[...].astype(F32) + stem_bias[...]
    centred = centred - jnp.mean(centred, axis=1, keepdims=True)
    position[...] = (centred * ln1_gain[...]).astype(BF16)

    def rows_of(which):
        return pl.ds(pl.multiple_of(which * share, share), share)

    def part_copy(source, peer):
        return remote(
            part_send.at[peer],
            part.at[source, rows_of(replica)],
            part_send_sem.at[0, peer],
            part_recv_sem.at[0, source],
            ctx=peer,
        )

    def relay(hop, source, owner, target):
        piece = part.at[source, rows_of(owner)]
        return remote(
            piece, piece, part_send_sem.at[hop, source], part_recv_sem.at[hop, source], dp=target
        )

    for copy in tables:
        copy.wait()
    planes = jnp.concatenate([(logs[a] - level).astype(BF16) for a in range(STRIDE)], axis=1)
    picked = jnp.dot(select[...], planes, preferred_element_type=F32).astype(BF16)
    picked = [picked[b * tokens : (b + 1) * tokens] * keep[...] for b in range(STRIDE)]
    folded = jnp.dot(jnp.concatenate(picked, axis=1), fold[...], preferred_element_type=F32)
    half = tokens // 2
    folded = folded[0:half, 0:lanes] + folded[half:, lanes:]
    blocks_send[...] = folded.astype(BF16)
    blocks[me] = folded.astype(BF16)

    def blocks_copy(slot, peer):
        return remote(
            blocks_send,
            blocks.at[me],
            blocks_send_sem.at[slot],
            blocks_recv_sem.at[me],
            ctx=peer,
        )

    def blocks_relay(source, slot):
        return remote(
            blocks.at[source],
            blocks.at[source],
            blocks_send_sem.at[slot],
            blocks_recv_sem.at[source],
            ctx=twin,
        )

    pl.semaphore_wait(barrier, n + 1)
    each_peer(lambda peer: sum_copy(me, peer).start())
    corner = me - 1 + 2 * my_side
    inside = (1 - my_side) * ((me + n - 1) // n) + my_side * ((2 * n - 2 - me) // n)

    @pl.when(inside == 1)
    def _():
        blocks_copy(pairs, corner).start()

    blocks_copy(pairs - 1, twin).start()
    for step in range(pairs - 1):
        blocks_copy(step, 2 * pair_at(step) + my_side).start()

    for piece in range(4):
        qkv_copy(piece).wait()
    rows = position[rows_of(replica), :]
    for kind in range(3):
        result = jnp.dot(
            rows, w_qkv[:, kind * width : (kind + 1) * width], preferred_element_type=F32
        ).astype(BF16)
        for peer in range(n):
            part_send[peer, :, kind * lanes : (kind + 1) * lanes] = result[
                :, peer * lanes : (peer + 1) * lanes
            ]
    for mask in range(1, n):
        part_copy(me, partner(me, mask, n)).start()
    for copy in weights:
        copy.start()

    def my_lanes(kind):
        return pl.ds(pl.multiple_of(kind * width + me * lanes, lanes), lanes)

    mine = jnp.concatenate([w_qkv[:, my_lanes(kind)] for kind in range(3)], axis=1)
    part[me] = jnp.dot(position[...], mine, preferred_element_type=F32).astype(BF16)
    taps = stem_weight.shape[0]
    kernel_raw[...] = jnp.zeros(kernel_raw.shape, BF16)
    kernel_raw[0:taps, :] = stem_weight[...]
    kernel_mixed[...] = jnp.zeros(kernel_mixed.shape, BF16)
    kernel = stem_weight[...].astype(F32)
    kernel = (kernel - jnp.mean(kernel, axis=1, keepdims=True)) * ln1_gain[...]
    kernel_mixed[0:taps, :] = kernel.astype(BF16)
    high = ln1_bias[...].astype(BF16)
    low = (ln1_bias[...] - high.astype(F32)).astype(BF16)
    line = iota((8, width), 0)
    bias_rows = jnp.where(line == 0, high.astype(F32), jnp.where(line == 1, low.astype(F32), 0.0))
    kernel_mixed[taps : taps + 8, :] = bias_rows.astype(BF16)
    mixing = jnp.dot(kernel_mixed[...], mine, preferred_element_type=F32)
    shift = mixing[taps : taps + 1] + mixing[taps + 1 : taps + 2]
    my_bias = [qkv_bias[:, my_lanes(kind)] for kind in range(3)]
    shift = shift + jnp.concatenate(my_bias, axis=1)
    mixing = mixing.astype(BF16)

    def relay_first(*masks):
        for mask in masks:
            source = partner(me, mask, n)
            part_copy(source, source).wait_recv()
            relay(1, source, replica, near).start()
            relay(2, source, replica, across).start()

    def relay_second(*masks):
        for mask in masks:
            source = partner(me, mask, n)
            relay(2, source, across, across).wait_recv()
            relay(3, source, across, near).start()

    each_peer(lambda peer: sum_copy(peer, peer).wait_recv())
    blocks_relay(twin, 0).wait_recv()

    @pl.when(inside == 1)
    def _():
        blocks_relay(corner, 0).wait_recv()

    log_mean = jnp.log(jnp.sum(sum_got[...], axis=0)[0:1, 0:1] / cells)

    def spread_windows(t):
        packed = blocks[t].astype(F32) + (sum_got[t][1:2, 0:1] - log_mean)
        spread = jnp.concatenate([packed, pltpu.roll(packed, lanes // 2, 1)], axis=0)
        column = iota(spread.shape, 0) & (grid - 1)
        before = jnp.where(column == 0, 0.0, pltpu.roll(spread, 1, 0))
        after = jnp.where(column == grid - 1, 0.0, pltpu.roll(spread, tokens - 1, 0))
        wide = jnp.concatenate([v.astype(BF16) for v in (spread, before, after)], axis=1)
        edge = jnp.zeros((grid, wide.shape[1]), BF16)
        above = jnp.concatenate([edge, wide[: tokens - grid]], axis=0)
        below = jnp.concatenate([wide[grid:], edge], axis=0)
        wide = jnp.concatenate([wide, above, below], axis=1)
        windows[t] = jnp.dot(wide, expand[...], preferred_element_type=F32).astype(BF16)

    for t in (me, twin, me + inside * (2 * my_side - 1)):
        spread_windows(t)

    tap = iota((tokens, 256), 1)
    face = KERNEL * KERNEL

    def patches_of(before, here, after):
        inner = jnp.where(tap < taps - face, here, after)
        return jnp.where(tap < face, before, inner)

    before = windows[me - (me + n - 1) // n]
    after = windows[me + (2 * n - 2 - me) // n]
    before = jnp.where(me > 0, before, jnp.zeros_like(before))
    after = jnp.where(me < n - 1, after, jnp.zeros_like(after))
    patches = patches_of(before, windows[me], after)
    embedded = jnp.dot(patches, kernel_raw[...], preferred_element_type=F32)
    embedded = embedded + stem_bias[...] + pos_embed[...].astype(F32)
    residual[...] = embedded.astype(BF16)
    centre = residual[...].astype(F32)
    centre = centre - jnp.mean(centre, axis=1, keepdims=True)
    inverse = lax.rsqrt(jnp.mean(centre * centre, axis=1, keepdims=True) + 1e-06)
    inverse = jnp.broadcast_to(inverse, (tokens, lanes))
    stats = [inverse[i * lanes : (i + 1) * lanes].T[0:1] for i in range(tokens // lanes)]
    stats.append(jnp.zeros((8 - len(stats), lanes), F32))
    stats = jnp.concatenate(stats, axis=0)
    stats_send[...] = stats
    stats_got[me] = stats

    def stats_copy(source, peer):
        return remote(
            stats_send,
            stats_got.at[source],
            stats_send_sem.at[peer],
            stats_recv_sem.at[source],
            ctx=peer,
        )

    each_peer(lambda peer: stats_copy(me, peer).start())

    twin_corner = twin + 1 - 2 * my_side
    for step in range(pairs - 1):
        source = 2 * pair_at(step) + my_side
        blocks_relay(source, 0).wait_recv()

        @pl.when(source != twin_corner)
        def _():
            blocks_relay(source, pairs + 1 + step).start()

    relay_first(*range(1, n // 2))
    for step in range(pairs - 1):
        source = 2 * pair_at(step) + 1 - my_side

        @pl.when(source != corner)
        def _():
            blocks_relay(source, 0).wait_recv()

    for mask in range(2, n):
        spread_windows(partner(me, mask, n))
    lag = n // 2 - 2
    for mask in range(1, n + lag):
        if n // 2 <= mask < n:
            relay_first(mask)
        if mask > lag:
            relay_second(mask - lag)

    each_peer(lambda peer: stats_copy(peer, peer).wait_recv())

    def arrived(source):
        relay(1, source, near, near).wait_recv()
        relay(3, source, diagonal, near).wait_recv()

    each_peer(arrived)

    scales = (1.0 / head_size**0.5, 1.0, 1.0)
    for t in range(n):
        nothing = jnp.zeros((tokens, 256), BF16)
        patches = patches_of(
            windows[t - 1] if t > 0 else nothing,
            windows[t],
            windows[t + 1] if t < n - 1 else nothing,
        )
        result = jnp.dot(patches, mixing, preferred_element_type=F32) + part[t].astype(F32)
        inverse = jnp.concatenate(
            [
                jnp.broadcast_to(stats_got[t, i : i + 1, :], (lanes, lanes)).T
                for i in range(tokens // lanes)
            ],
            axis=0,
        )
        for kind, scale in enumerate(scales):
            columns = slice(kind * lanes, (kind + 1) * lanes)
            rows = result[:, columns] * inverse + shift[:, columns]
            if kind == 0:
                query[t] = (rows * scale).astype(BF16)
            elif kind == 1:
                key[:, t * tokens : (t + 1) * tokens] = rows.T.astype(BF16)
            else:
                value_wide[t * tokens : (t + 1) * tokens, 0:lanes] = rows.astype(BF16)
    keys_total = n * tokens
    value_wide[:, lanes:] = jnp.ones((keys_total, lanes), BF16)

    rows = min(tokens, ROWS)
    halves = range(tokens // rows)

    def mixed_copy(half, source, peer):
        return remote(
            mixed_send.at[half, peer],
            mixed_got.at[half, source],
            mixed_send_sem.at[half, peer],
            mixed_recv_sem.at[half, source],
            ctx=peer,
        )

    batch = n // 2

    def attend(turn, carry):
        half = lax.rem(turn, len(halves))
        peers = [partner(me, n - 1 - turn // len(halves) * batch - i, n) for i in range(batch)]
        mine_rows = pl.ds(pl.multiple_of(half * rows, rows), rows)
        lane = iota((rows, lanes), 1) // head_size
        for peer in peers:
            picked = query[peer, mine_rows, :]
            mixed = None
            for head in range(local_heads):
                mine = jnp.where(lane == head, picked, jnp.zeros_like(picked))
                scores = jnp.dot(mine, key[...], preferred_element_type=F32)
                weight = jnp.exp(scores - jnp.max(scores, axis=1, keepdims=True))
                product = jnp.dot(
                    weight.astype(BF16), value_wide[...], preferred_element_type=F32
                )
                product = product[:, 0:lanes] / product[:, lanes:]
                mixed = product if mixed is None else jnp.where(lane == head, product, mixed)
            mixed_send[half, peer] = mixed.astype(BF16)
        for i, peer in enumerate(peers):
            if i < batch - 1:
                mixed_copy(half, me, peer).start()
            else:

                @pl.when(turn < len(halves))
                def _():
                    mixed_copy(half, me, peer).start()

        return carry

    lax.fori_loop(0, 2 * len(halves), attend, 0)
    for half in halves:
        mixed_got[half, me] = mixed_send[half, me]

    hidden_width = w_fc1.shape[1]
    tile = math.gcd(hidden_width, 512)
    for copy in weights:
        copy.wait()
    for half in halves:
        each_peer(lambda peer: mixed_copy(half, peer, peer).wait_recv())
    attended = jnp.concatenate(
        [
            jnp.concatenate([mixed_got[half, piece] for piece in range(n)], axis=1)
            for half in halves
        ],
        axis=0,
    )
    stream = (
        residual[...].astype(F32)
        + jnp.dot(attended, w_out[...], preferred_element_type=F32)
        + out_bias[...]
    ).astype(BF16)
    stream = stream.astype(F32)
    normed[...] = norm_rows(stream, ln2_gain[...], ln2_bias[...]).astype(BF16)
    total[...] = stream + fc2_bias[...]
    for start in range(0, hidden_width, tile):
        columns = slice(start, start + tile)
        hidden = jnp.dot(normed[...], w_fc1[:, columns], preferred_element_type=F32)
        hidden = hidden + fc1_bias[:, columns]
        hidden = 0.5 * hidden * (1.0 + lax.erf(hidden * math.sqrt(0.5)))
        total[...] += jnp.dot(hidden.astype(BF16), w_fc2[columns, :], preferred_element_type=F32)
    encoded[...] = total[...].astype(BF16)

    def finish(peer):
        sum_copy(me, peer).wait_send()
        stats_copy(me, peer).wait_send()
        part_copy(me, peer).wait_send()
        for half in halves:
            mixed_copy(half, me, peer).wait_send()
        relay(1, peer, replica, near).wait_send()
        relay(2, peer, replica, across).wait_send()
        relay(3, peer, across, near).wait_send()

    each_peer(finish)
    for step in range(pairs - 1):
        source = 2 * pair_at(step) + my_side
        blocks_copy(step, source).wait_send()

        @pl.when(source != twin_corner)
        def _():
            blocks_relay(source, pairs + 1 + step).wait_send()

    blocks_copy(pairs - 1, twin).wait_send()

    @pl.when(inside == 1)
    def _():
        blocks_copy(pairs, corner).wait_send()


def shared_call(
    density,
    stem_weight,
    stem_bias,
    pos_embed,
    ln1_gain,
    ln1_bias,
    w_qkv,
    qkv_bias,
    w_out,
    out_bias,
    ln2_gain,
    ln2_bias,
    w_fc1,
    fc1_bias,
    w_fc2,
    fc2_bias,
):
    n = lax.axis_size("ctx")
    tokens, width = pos_embed.shape
    side = density.shape[1]
    vmem = pl.BlockSpec(memory_space=pltpu.VMEM)
    hbm = pl.BlockSpec(memory_space=pl.ANY)
    tables = stem_tables(side, stem_weight.shape[0])

    def line(vector):
        return vector.reshape(1, -1)

    dma = pltpu.SemaphoreType.DMA
    lanes = 128
    pairs = n // 2
    return pl.pallas_call(
        functools.partial(shared_kernel, n, (density.shape[0] * side * side) * n),
        out_shape=jax.ShapeDtypeStruct((tokens, width), BF16),
        in_specs=[
            vmem, vmem, vmem, vmem, vmem, vmem, hbm, vmem,
            hbm, vmem, vmem, vmem, hbm, vmem, hbm, vmem,
            hbm, hbm, hbm, hbm,
        ],
        out_specs=vmem,
        scratch_shapes=[
            pltpu.VMEM(w_qkv.shape, BF16),
            pltpu.VMEM(w_out.shape, BF16),
            pltpu.VMEM(w_fc1.shape, BF16),
            pltpu.VMEM(w_fc2.shape, BF16),
            *[pltpu.VMEM(table.shape, BF16) for table in tables],
            dma((4,)),
            dma((3,)),
            dma((4,)),
            pltpu.VMEM((8, lanes), F32),
            pltpu.VMEM((n, 8, lanes), F32),
            pltpu.VMEM((8, lanes), F32),
            pltpu.VMEM((n, 8, lanes), F32),
            pltpu.VMEM((tokens // 2, lanes), BF16),
            pltpu.VMEM((n, tokens // 2, lanes), BF16),
            pltpu.VMEM((n, tokens, 256), BF16),
            pltpu.VMEM((256, width), BF16),
            pltpu.VMEM((256, width), BF16),
            pltpu.VMEM((tokens, width), BF16),
            pltpu.VMEM((tokens, width), BF16),
            pltpu.VMEM((tokens, width), BF16),
            pltpu.VMEM((n, tokens // 4, 3 * lanes), BF16),
            pltpu.VMEM((n, tokens, 3 * lanes), BF16),
            pltpu.VMEM((n, tokens, lanes), BF16),
            pltpu.VMEM((lanes, n * tokens), BF16),
            pltpu.VMEM((n * tokens, 2 * lanes), BF16),
            pltpu.VMEM((tokens // ROWS, n, ROWS, lanes), BF16),
            pltpu.VMEM((tokens // ROWS, n, ROWS, lanes), BF16),
            pltpu.VMEM((tokens, width), F32),
            dma((n,)),
            dma((n,)),
            dma((n,)),
            dma((n,)),
            dma((2 * pairs + 1,)),
            dma((n,)),
            dma((4, n)),
            dma((4, n)),
            dma((tokens // ROWS, n)),
            dma((tokens // ROWS, n)),
        ],
        compiler_params=pltpu.CompilerParams(
            collective_id=1, has_side_effects=True, vmem_limit_bytes=60 * 1024 * 1024
        ),
    )(
        density,
        stem_weight,
        line(stem_bias),
        pos_embed,
        line(ln1_gain),
        line(ln1_bias),
        w_qkv,
        line(qkv_bias),
        w_out,
        line(out_bias),
        line(ln2_gain),
        line(ln2_bias),
        w_fc1,
        line(fc1_bias),
        w_fc2,
        line(fc2_bias),
        *tables,
    )


def per_device(
    density,
    stem_weight,
    stem_bias,
    pos_embed,
    ln1_gain,
    ln1_bias,
    w_qkv,
    qkv_bias,
    w_out,
    out_bias,
    ln2_gain,
    ln2_bias,
    w_fc1,
    fc1_bias,
    w_fc2,
    fc2_bias,
):
    n = lax.axis_size("ctx")
    tokens, width = pos_embed.shape
    if shares_positions(n, lax.axis_size("dp"), density, pos_embed):
        return shared_call(
            density, stem_weight, stem_bias, pos_embed, ln1_gain, ln1_bias, w_qkv, qkv_bias,
            w_out, out_bias, ln2_gain, ln2_bias, w_fc1, fc1_bias, w_fc2, fc2_bias,
        )
    hidden_width = w_fc1.shape[1]
    planes, side, _ = density.shape
    assert planes == STRIDE and tokens == (side // STRIDE) ** 2
    head_size = width // HEADS
    local_heads = max(HEADS // n, 1)
    groups = max(n // HEADS, 1)
    head_groups = HEADS // local_heads
    group_width = local_heads * head_size
    share = tokens // groups
    pair = 2 * side
    window = planes + 2
    vmem = pl.BlockSpec(memory_space=pltpu.VMEM)
    hbm = pl.BlockSpec(memory_space=pl.ANY)

    def line(vector):
        return vector.reshape(1, -1)

    dma = pltpu.SemaphoreType.DMA
    wide_shape = (n * tokens, 2 * group_width) if group_width % 128 == 0 else (16, 128)
    return pl.pallas_call(
        functools.partial(layer_kernel, n, density.size * n),
        out_shape=jax.ShapeDtypeStruct((tokens, width), BF16),
        in_specs=[
            vmem, vmem, vmem, vmem, vmem, vmem, hbm, vmem,
            hbm, vmem, vmem, vmem, hbm, vmem, hbm, vmem,
        ],
        out_specs=vmem,
        scratch_shapes=[
            pltpu.VMEM(w_qkv.shape, BF16),
            pltpu.VMEM(w_out.shape, BF16),
            pltpu.VMEM(w_fc1.shape, BF16),
            pltpu.VMEM(w_fc2.shape, BF16),
            dma((4,)),
            pltpu.VMEM((2, side, side), F32),
            pltpu.VMEM((8, 128), F32),
            pltpu.VMEM((n, 8, 128), F32),
            dma((2,)),
            dma((2,)),
            dma((n,)),
            dma((n,)),
            pltpu.VMEM((KERNEL, tokens, side), BF16),
            pltpu.VMEM((KERNEL, window * pair, 256), BF16),
            pltpu.VMEM((side, window * pair), BF16),
            pltpu.VMEM((256, width), BF16),
            pltpu.VMEM((tokens, width), BF16),
            pltpu.VMEM((tokens, width), BF16),
            pltpu.VMEM((3, head_groups, tokens, group_width), BF16),
            pltpu.VMEM((n, share, group_width), BF16),
            pltpu.VMEM((n, tokens, group_width), BF16),
            pltpu.VMEM((n, tokens, group_width), BF16),
            pltpu.VMEM(wide_shape, BF16),
            pltpu.VMEM((n, share, group_width), BF16),
            pltpu.VMEM((n, share, group_width), BF16),
            pltpu.VMEM((tokens, width), BF16),
            pltpu.VMEM((tokens, width), F32),
            dma((4, n)),
            dma((4, n)),
        ],
        compiler_params=pltpu.CompilerParams(
            collective_id=0, has_side_effects=True, vmem_limit_bytes=60 * 1024 * 1024
        ),
    )(
        density,
        stem_weight,
        line(stem_bias),
        pos_embed,
        line(ln1_gain),
        line(ln1_bias),
        w_qkv,
        line(qkv_bias),
        w_out,
        line(out_bias),
        line(ln2_gain),
        line(ln2_bias),
        w_fc1,
        line(fc1_bias),
        w_fc2,
        line(fc2_bias),
    )


def solution(mesh):
    in_specs = (P(("dp", "ctx"), None, None), P(), P(), P("ctx", None)) + (P(),) * 12
    return jax.shard_map(
        per_device,
        mesh=mesh,
        in_specs=in_specs,
        out_specs=P(("dp", "ctx"), None),
        check_vma=False,
    )
```

```python
import functools
import math

import jax
import jax.numpy as jnp
import numpy as np
from jax import lax
from jax.experimental import pallas as pl
from jax.experimental.pallas import tpu as pltpu
from jax.sharding import PartitionSpec as P

HEADS = 16
KERNEL = 6
STRIDE = 4
ROWS = 128
MESH = pl.DeviceIdType.MESH
F32 = jnp.float32
BF16 = jnp.bfloat16


def iota(shape, axis):
    return lax.broadcasted_iota(jnp.int32, shape, axis)


def partner(me, mask, n):
    result, bit = 0, 1
    while bit < n:
        result += ((me // bit + mask // bit) % 2) * bit
        bit *= 2
    return result


def norm_rows(values, gain_vector, shift_vector):
    center = values - jnp.mean(values, axis=-1, keepdims=True)
    spread = jnp.mean(center * center, axis=-1, keepdims=True)
    return center * lax.rsqrt(spread + 1e-06) * gain_vector + shift_vector


def layer_kernel(
    n,
    cells,
    density,
    stem_weight,
    stem_bias,
    pos_embed,
    ln1_gain,
    ln1_bias,
    w_qkv_hbm,
    qkv_bias,
    w_out_hbm,
    out_bias,
    ln2_gain,
    ln2_bias,
    w_fc1_hbm,
    fc1_bias,
    w_fc2_hbm,
    fc2_bias,
    encoded,
    w_qkv,
    w_out,
    w_fc1,
    w_fc2,
    weight_sem,
    halo,
    sum_send,
    sum_got,
    edge_send_sem,
    edge_recv_sem,
    sum_send_sem,
    sum_recv_sem,
    select_rows,
    fold,
    planes_wide,
    kernel_rows,
    residual,
    normed,
    outgoing,
    query_got,
    key_got,
    value_got,
    value_wide,
    mixed_send,
    mixed_got,
    attended,
    total,
    send_sem,
    recv_sem,
):
    me = lax.axis_index("ctx")
    planes, side, _ = density.shape
    tokens, width = residual.shape
    head_size = width // HEADS
    local_heads = max(HEADS // n, 1)
    groups = max(n // HEADS, 1)
    group_width = local_heads * head_size
    share = tokens // groups
    grid = side // STRIDE
    window = planes + 2

    weights = [
        pltpu.make_async_copy(source, target, weight_sem.at[i])
        for i, (source, target) in enumerate(
            ((w_qkv_hbm, w_qkv), (w_out_hbm, w_out), (w_fc1_hbm, w_fc1), (w_fc2_hbm, w_fc2))
        )
    ]
    for copy in weights:
        copy.start()

    barrier = pltpu.get_barrier_semaphore()

    def each_peer(action):
        def step(offset, carry):
            action(partner(me, n - offset, n))
            return carry

        lax.fori_loop(1, n, step, 0)

    each_peer(
        lambda peer: pl.semaphore_signal(
            barrier, inc=1, device_id={"ctx": peer}, device_id_type=MESH
        )
    )

    own = jnp.sum(density[...], axis=0)
    own = jnp.sum(own, axis=(0, 1), keepdims=True)
    sum_send[...] = jnp.broadcast_to(own, sum_send.shape)
    sum_got[me] = jnp.broadcast_to(own, sum_send.shape)

    @pl.when(me == 0)
    def _():
        halo[0] = jnp.ones((side, side), F32)

    @pl.when(me == n - 1)
    def _():
        halo[1] = jnp.ones((side, side), F32)

    pl.semaphore_wait(barrier, n - 1)

    def edge(side_index, plane, peer):
        return pltpu.make_async_remote_copy(
            src_ref=density.at[plane],
            dst_ref=halo.at[side_index],
            send_sem=edge_send_sem.at[side_index],
            recv_sem=edge_recv_sem.at[side_index],
            device_id={"ctx": peer},
            device_id_type=MESH,
        )

    up = edge(0, planes - 1, lax.rem(me + 1, n))
    down = edge(1, 0, lax.rem(me + n - 1, n))

    def sum_copy(source, peer):
        return pltpu.make_async_remote_copy(
            src_ref=sum_send,
            dst_ref=sum_got.at[source],
            send_sem=sum_send_sem.at[peer],
            recv_sem=sum_recv_sem.at[source],
            device_id={"ctx": peer},
            device_id_type=MESH,
        )

    each_peer(lambda peer: sum_copy(me, peer).start())

    @pl.when(me < n - 1)
    def _():
        up.start()

    @pl.when(me > 0)
    def _():
        down.start()

    pair = 2 * side
    row = iota((tokens, side), 0)
    col = iota((tokens, side), 1)
    for b in range(KERNEL):
        hit = col == STRIDE * (row // grid) - 1 + b
        select_rows[b] = jnp.where(hit, 1.0, 0.0).astype(BF16)
    lane_row = iota((pair, 256), 0)
    lane_col = iota((pair, 256), 1)
    high = lane_row // side
    offset_c = ((lane_row + 1) & (STRIDE - 1)) + STRIDE * high
    for b in range(KERNEL):
        for a in range(window):
            hit = (offset_c < KERNEL) & (lane_col == (a * KERNEL + b) * KERNEL + offset_c)
            fold[b, a * pair : (a + 1) * pair, :] = jnp.where(hit, 1.0, 0.0).astype(BF16)
    taps = stem_weight.shape[0]
    kernel_rows[...] = jnp.zeros(kernel_rows.shape, BF16)
    kernel_rows[0:taps, :] = stem_weight[...]
    tile_row = iota((tokens, pair), 0)
    tile_lane = iota((tokens, pair), 1)
    keep = (((tile_lane & (side - 1)) + 1) // STRIDE - tile_lane // side) == (
        tile_row & (grid - 1)
    )
    keep = jnp.where(keep, 1.0, 0.0).astype(BF16)

    each_peer(lambda peer: sum_copy(peer, peer).wait_recv())

    @pl.when(me > 0)
    def _():
        up.wait_recv()

    @pl.when(me < n - 1)
    def _():
        down.wait_recv()

    mean_density = (jnp.sum(sum_got[...], axis=0)[0:1, 0:1]) / cells
    for a in range(window):
        if a == 0:
            plane = jnp.where(me > 0, jnp.log(halo[0] / mean_density), 0.0)
        elif a == window - 1:
            plane = jnp.where(me < n - 1, jnp.log(halo[1] / mean_density), 0.0)
        else:
            plane = jnp.log(density[a - 1] / mean_density)
        plane = plane.astype(BF16)
        planes_wide[:, a * pair : (a + 1) * pair] = jnp.concatenate([plane, plane], axis=1)

    keep_wide = jnp.concatenate([keep] * window, axis=1)
    patches = jnp.zeros((tokens, 256), F32)
    for b in range(KERNEL):
        rows = jnp.dot(select_rows[b], planes_wide[...], preferred_element_type=F32)
        rows = rows.astype(BF16) * keep_wide
        patches += jnp.dot(rows, fold[b], preferred_element_type=F32)
    embedded = jnp.dot(patches.astype(BF16), kernel_rows[...], preferred_element_type=F32)
    embedded = embedded + stem_bias[...] + pos_embed[...].astype(F32)
    residual[...] = embedded.astype(BF16)
    normed[...] = norm_rows(residual[...].astype(F32), ln1_gain[...], ln1_bias[...]).astype(BF16)

    def head_group(peer):
        return peer // groups

    def my_rows(peer):
        return pl.ds(pl.multiple_of(lax.rem(peer, groups) * share, share), share)

    def projected_copy(kind, source, peer):
        piece = outgoing.at[kind, head_group(peer)]
        got = (query_got, key_got, value_got)[kind]
        if kind == 0:
            piece = piece.at[my_rows(peer)]
        return pltpu.make_async_remote_copy(
            src_ref=piece,
            dst_ref=got.at[source],
            send_sem=send_sem.at[kind, peer],
            recv_sem=recv_sem.at[kind, source],
            device_id={"ctx": peer},
            device_id_type=MESH,
        )

    weights[0].wait()
    block = 256
    for kind in (1, 2, 0):
        for start in range(0, width, block):
            columns = slice(kind * width + start, kind * width + start + block)
            result = jnp.dot(normed[...], w_qkv[:, columns], preferred_element_type=F32)
            result = result + qkv_bias[:, columns]
            if kind == 0:
                result = result * (1.0 / head_size**0.5)
            result = result.astype(BF16)
            for part in range(block // group_width):
                outgoing[kind, start // group_width + part] = result[
                    :, part * group_width : (part + 1) * group_width
                ]
        each_peer(lambda peer: projected_copy(kind, me, peer).start())
    query_got[me] = outgoing[0, head_group(me), my_rows(me), :]
    key_got[me] = outgoing[1, head_group(me)]
    value_got[me] = outgoing[2, head_group(me)]

    each_peer(lambda peer: projected_copy(1, peer, peer).wait_recv())
    each_peer(lambda peer: projected_copy(2, peer, peer).wait_recv())

    keys_total = n * tokens
    wide = group_width % 128 == 0
    if wide:
        value_wide[:, 0:group_width] = value_got[...].reshape(keys_total, group_width)
        value_wide[:, group_width:] = jnp.ones((keys_total, group_width), BF16)

    def mixed_copy(source, peer):
        return pltpu.make_async_remote_copy(
            src_ref=mixed_send.at[peer],
            dst_ref=mixed_got.at[source],
            send_sem=send_sem.at[3, peer],
            recv_sem=recv_sem.at[3, source],
            device_id={"ctx": peer},
            device_id_type=MESH,
        )

    def attend(offset, carry):
        peer = partner(me, lax.rem(n - offset, n), n)

        @pl.when(offset > 0)
        def _():
            projected_copy(0, peer, peer).wait_recv()

        rows = min(share, ROWS)
        for first in range(0, share, rows):
            query = query_got[peer, first : first + rows, :]
            lane = iota((rows, group_width), 1) // head_size
            mixed = None
            for head in range(local_heads):
                mine = query
                if local_heads > 1:
                    mine = jnp.where(lane == head, query, jnp.zeros_like(query))
                scores = lax.dot_general(
                    mine,
                    key_got[...].reshape(keys_total, group_width),
                    (((1,), (1,)), ((), ())),
                    preferred_element_type=F32,
                )
                weight = jnp.exp(scores - jnp.max(scores, axis=1, keepdims=True))
                values = value_wide[...] if wide else value_got[...].reshape(keys_total, group_width)
                product = jnp.dot(weight.astype(BF16), values, preferred_element_type=F32)
                if wide:
                    part = product[:, 0:group_width] / product[:, group_width:]
                else:
                    part = product / jnp.sum(weight, axis=1, keepdims=True)
                mixed = part if mixed is None else jnp.where(lane == head, part, mixed)
            mixed_send[peer, first : first + rows, :] = mixed.astype(BF16)

        @pl.when(offset > 0)
        def _():
            mixed_copy(me, peer).start()

        @pl.when(offset == 0)
        def _():
            mixed_got[me] = mixed_send[me]

        return carry

    lax.fori_loop(0, n, attend, 0)

    each_peer(lambda peer: mixed_copy(peer, peer).wait_recv())
    for piece in range(n):
        first = (piece % groups) * share
        column = (piece // groups) * group_width
        attended[first : first + share, column : column + group_width] = mixed_got[piece]

    weights[1].wait()
    stream = (
        residual[...].astype(F32)
        + jnp.dot(attended[...], w_out[...], preferred_element_type=F32)
        + out_bias[...]
    ).astype(BF16)
    residual[...] = stream
    stream = stream.astype(F32)
    normed[...] = norm_rows(stream, ln2_gain[...], ln2_bias[...]).astype(BF16)
    total[...] = stream + fc2_bias[...]

    weights[2].wait()
    weights[3].wait()
    hidden_width = w_fc1.shape[1]
    tile = math.gcd(hidden_width, 512)
    for start in range(0, hidden_width, tile):
        columns = slice(start, start + tile)
        hidden = jnp.dot(normed[...], w_fc1[:, columns], preferred_element_type=F32)
        hidden = hidden + fc1_bias[:, columns]
        hidden = 0.5 * hidden * (1.0 + lax.erf(hidden * math.sqrt(0.5)))
        total[...] += jnp.dot(hidden.astype(BF16), w_fc2[columns, :], preferred_element_type=F32)
    encoded[...] = total[...].astype(BF16)

    def finish(peer):
        sum_copy(me, peer).wait_send()
        for kind in range(3):
            projected_copy(kind, me, peer).wait_send()
        mixed_copy(me, peer).wait_send()

    each_peer(finish)

    @pl.when(me < n - 1)
    def _():
        up.wait_send()

    @pl.when(me > 0)
    def _():
        down.wait_send()


def stem_tables(side, features):
    grid = side // STRIDE
    tokens = grid * grid
    token = np.arange(tokens)
    select = np.zeros((STRIDE, tokens, side), np.float32)
    for b in range(STRIDE):
        select[b, token, STRIDE * (token // grid) + b] = 1
    x = np.arange(side)
    keep = np.tile(x[None, :] // STRIDE == token[:, None] % grid, (1, STRIDE))
    fold = np.zeros((STRIDE, STRIDE, side, 256), np.float32)
    for b in range(STRIDE):
        for a in range(STRIDE):
            lane = (a * STRIDE + b) * STRIDE + x % STRIDE
            fold[b, a, x, lane] = 1
            fold[b, a, x, 192 + lane] = 1
    expand = np.zeros((3, 3, 128, 256), np.float32)
    shifts = {0: 0, -1: 1, 1: 2}
    for a in range(KERNEL):
        for b in range(KERNEL):
            for c in range(KERNEL):
                block = ((a - 1) % STRIDE * STRIDE + (b - 1) % STRIDE) * STRIDE + (c - 1) % STRIDE
                lane = (a * KERNEL + b) * KERNEL + c
                expand[shifts[(b - 1) // STRIDE], shifts[(c - 1) // STRIDE], block, lane] = 1
    return [
        jnp.asarray(table.reshape(-1, table.shape[-1]), BF16)
        for table in (select, keep.astype(np.float32), fold, expand)
    ]


def shares_positions(n, replicas, density, pos_embed):
    planes, side, _ = density.shape
    tokens, width = pos_embed.shape
    return (
        replicas == 4
        and n % 2 == 0
        and n <= HEADS
        and (HEADS // n) * (width // HEADS) == 128
        and planes == STRIDE
        and side == 64
        and tokens == (side // STRIDE) ** 2
    )


def shared_kernel(
    n,
    cells,
    density,
    stem_weight,
    stem_bias,
    pos_embed,
    ln1_gain,
    ln1_bias,
    w_qkv_hbm,
    qkv_bias,
    w_out_hbm,
    out_bias,
    ln2_gain,
    ln2_bias,
    w_fc1_hbm,
    fc1_bias,
    w_fc2_hbm,
    fc2_bias,
    select_hbm,
    keep_hbm,
    fold_hbm,
    expand_hbm,
    encoded,
    w_qkv,
    w_out,
    w_fc1,
    w_fc2,
    select,
    keep,
    fold,
    expand,
    qkv_sem,
    weight_sem,
    table_sem,
    sum_send,
    sum_got,
    stats_send,
    stats_got,
    blocks_send,
    blocks,
    windows,
    kernel_raw,
    kernel_mixed,
    position,
    residual,
    normed,
    part_send,
    part,
    query,
    key,
    value_wide,
    mixed_send,
    mixed_got,
    total,
    sum_send_sem,
    sum_recv_sem,
    stats_send_sem,
    stats_recv_sem,
    blocks_send_sem,
    blocks_recv_sem,
    part_send_sem,
    part_recv_sem,
    mixed_send_sem,
    mixed_recv_sem,
):
    me = lax.axis_index("ctx")
    replica = lax.axis_index("dp")
    near = replica + 1 - 2 * lax.rem(replica, 2)
    across = lax.rem(replica + 2, 4)
    diagonal = lax.rem(near + 2, 4)
    tokens, width = residual.shape
    side = density.shape[1]
    grid = side // STRIDE
    head_size = width // HEADS
    local_heads = HEADS // n
    lanes = 128
    share = tokens // 4
    pairs = n // 2
    my_pair, my_side = me // 2, lax.rem(me, 2)
    twin = 2 * my_pair + 1 - my_side

    def pair_at(step):
        return partner(my_pair, pairs - 1 - step, pairs)

    depth = width // 4

    def qkv_copy(piece):
        rows = pl.ds(piece * depth, depth)
        return pltpu.make_async_copy(w_qkv_hbm.at[rows], w_qkv.at[rows], qkv_sem.at[piece])

    tables = [
        pltpu.make_async_copy(source, target, table_sem.at[i])
        for i, (source, target) in enumerate(
            ((select_hbm, select), (keep_hbm, keep), (fold_hbm, fold), (expand_hbm, expand))
        )
    ]
    weights = [
        pltpu.make_async_copy(source, target, weight_sem.at[i])
        for i, (source, target) in enumerate(
            ((w_out_hbm, w_out), (w_fc1_hbm, w_fc1), (w_fc2_hbm, w_fc2))
        )
    ]
    for copy in tables:
        copy.start()
    for piece in range(4):
        qkv_copy(piece).start()

    barrier = pltpu.get_barrier_semaphore()

    def each_peer(action):
        def step(offset, carry):
            action(partner(me, n - offset, n))
            return carry

        lax.fori_loop(1, n, step, 0)

    each_peer(
        lambda peer: pl.semaphore_signal(
            barrier, inc=1, device_id={"ctx": peer}, device_id_type=MESH
        )
    )
    for other in (near, across):
        pl.semaphore_signal(barrier, inc=1, device_id={"dp": other}, device_id_type=MESH)

    def everywhere(values):
        return jnp.sum(jnp.sum(values, axis=0), axis=(0, 1), keepdims=True)

    logs = jnp.log(density[...])
    level = everywhere(logs) / (density.shape[0] * side * side)
    line = iota(sum_send.shape, 0)
    own = jnp.where(line == 0, everywhere(density[...]), level)
    sum_send[...] = own
    sum_got[me] = own
    def remote(source, target, send, recv, **device):
        return pltpu.make_async_remote_copy(
            src_ref=source,
            dst_ref=target,
            send_sem=send,
            recv_sem=recv,
            device_id=device,
            device_id_type=MESH,
        )

    def sum_copy(source, peer):
        return remote(
            sum_send, sum_got.at[source], sum_send_sem.at[peer], sum_recv_sem.at[source], ctx=peer
        )


    centred = pos_embed[...].astype(F32) + stem_bias[...]
    centred = centred - jnp.mean(centred, axis=1, keepdims=True)
    position[...] = (centred * ln1_gain[...]).astype(BF16)

    def rows_of(which):
        return pl.ds(pl.multiple_of(which * share, share), share)

    def part_copy(source, peer):
        return remote(
            part_send.at[peer],
            part.at[source, rows_of(replica)],
            part_send_sem.at[0, peer],
            part_recv_sem.at[0, source],
            ctx=peer,
        )

    def relay(hop, source, owner, target):
        piece = part.at[source, rows_of(owner)]
        return remote(
            piece, piece, part_send_sem.at[hop, source], part_recv_sem.at[hop, source], dp=target
        )

    for copy in tables:
        copy.wait()
    planes = jnp.concatenate([(logs[a] - level).astype(BF16) for a in range(STRIDE)], axis=1)
    picked = jnp.dot(select[...], planes, preferred_element_type=F32).astype(BF16)
    picked = [picked[b * tokens : (b + 1) * tokens] * keep[...] for b in range(STRIDE)]
    folded = jnp.dot(jnp.concatenate(picked, axis=1), fold[...], preferred_element_type=F32)
    half = tokens // 2
    folded = folded[0:half, 0:lanes] + folded[half:, lanes:]
    blocks_send[...] = folded.astype(BF16)
    blocks[me] = folded.astype(BF16)

    def blocks_copy(slot, peer):
        return remote(
            blocks_send,
            blocks.at[me],
            blocks_send_sem.at[slot],
            blocks_recv_sem.at[me],
            ctx=peer,
        )

    def blocks_relay(source, slot):
        return remote(
            blocks.at[source],
            blocks.at[source],
            blocks_send_sem.at[slot],
            blocks_recv_sem.at[source],
            ctx=twin,
        )

    pl.semaphore_wait(barrier, n + 1)
    each_peer(lambda peer: sum_copy(me, peer).start())
    corner = me - 1 + 2 * my_side
    inside = (1 - my_side) * ((me + n - 1) // n) + my_side * ((2 * n - 2 - me) // n)

    @pl.when(inside == 1)
    def _():
        blocks_copy(pairs, corner).start()

    blocks_copy(pairs - 1, twin).start()
    for step in range(pairs - 1):
        blocks_copy(step, 2 * pair_at(step) + my_side).start()

    for piece in range(4):
        qkv_copy(piece).wait()
    rows = position[rows_of(replica), :]
    for kind in range(3):
        result = jnp.dot(
            rows, w_qkv[:, kind * width : (kind + 1) * width], preferred_element_type=F32
        ).astype(BF16)
        for peer in range(n):
            part_send[peer, :, kind * lanes : (kind + 1) * lanes] = result[
                :, peer * lanes : (peer + 1) * lanes
            ]
    for mask in range(1, n):
        part_copy(me, partner(me, mask, n)).start()
    for copy in weights:
        copy.start()

    def my_lanes(kind):
        return pl.ds(pl.multiple_of(kind * width + me * lanes, lanes), lanes)

    mine = jnp.concatenate([w_qkv[:, my_lanes(kind)] for kind in range(3)], axis=1)
    part[me] = jnp.dot(position[...], mine, preferred_element_type=F32).astype(BF16)
    taps = stem_weight.shape[0]
    kernel_raw[...] = jnp.zeros(kernel_raw.shape, BF16)
    kernel_raw[0:taps, :] = stem_weight[...]
    kernel_mixed[...] = jnp.zeros(kernel_mixed.shape, BF16)
    kernel = stem_weight[...].astype(F32)
    kernel = (kernel - jnp.mean(kernel, axis=1, keepdims=True)) * ln1_gain[...]
    kernel_mixed[0:taps, :] = kernel.astype(BF16)
    high = ln1_bias[...].astype(BF16)
    low = (ln1_bias[...] - high.astype(F32)).astype(BF16)
    line = iota((8, width), 0)
    bias_rows = jnp.where(line == 0, high.astype(F32), jnp.where(line == 1, low.astype(F32), 0.0))
    kernel_mixed[taps : taps + 8, :] = bias_rows.astype(BF16)
    mixing = jnp.dot(kernel_mixed[...], mine, preferred_element_type=F32)
    shift = mixing[taps : taps + 1] + mixing[taps + 1 : taps + 2]
    my_bias = [qkv_bias[:, my_lanes(kind)] for kind in range(3)]
    shift = shift + jnp.concatenate(my_bias, axis=1)
    mixing = mixing.astype(BF16)

    def relay_first(*masks):
        for mask in masks:
            source = partner(me, mask, n)
            part_copy(source, source).wait_recv()
            relay(1, source, replica, near).start()
            relay(2, source, replica, across).start()

    def relay_second(*masks):
        for mask in masks:
            source = partner(me, mask, n)
            relay(2, source, across, across).wait_recv()
            relay(3, source, across, near).start()

    each_peer(lambda peer: sum_copy(peer, peer).wait_recv())
    blocks_relay(twin, 0).wait_recv()

    @pl.when(inside == 1)
    def _():
        blocks_relay(corner, 0).wait_recv()

    log_mean = jnp.log(jnp.sum(sum_got[...], axis=0)[0:1, 0:1] / cells)

    def spread_windows(t):
        packed = blocks[t].astype(F32) + (sum_got[t][1:2, 0:1] - log_mean)
        spread = jnp.concatenate([packed, pltpu.roll(packed, lanes // 2, 1)], axis=0)
        column = iota(spread.shape, 0) & (grid - 1)
        before = jnp.where(column == 0, 0.0, pltpu.roll(spread, 1, 0))
        after = jnp.where(column == grid - 1, 0.0, pltpu.roll(spread, tokens - 1, 0))
        wide = jnp.concatenate([v.astype(BF16) for v in (spread, before, after)], axis=1)
        edge = jnp.zeros((grid, wide.shape[1]), BF16)
        above = jnp.concatenate([edge, wide[: tokens - grid]], axis=0)
        below = jnp.concatenate([wide[grid:], edge], axis=0)
        wide = jnp.concatenate([wide, above, below], axis=1)
        windows[t] = jnp.dot(wide, expand[...], preferred_element_type=F32).astype(BF16)

    for t in (me, twin, me + inside * (2 * my_side - 1)):
        spread_windows(t)

    tap = iota((tokens, 256), 1)
    face = KERNEL * KERNEL

    def patches_of(before, here, after):
        inner = jnp.where(tap < taps - face, here, after)
        return jnp.where(tap < face, before, inner)

    before = windows[me - (me + n - 1) // n]
    after = windows[me + (2 * n - 2 - me) // n]
    before = jnp.where(me > 0, before, jnp.zeros_like(before))
    after = jnp.where(me < n - 1, after, jnp.zeros_like(after))
    patches = patches_of(before, windows[me], after)
    embedded = jnp.dot(patches, kernel_raw[...], preferred_element_type=F32)
    embedded = embedded + stem_bias[...] + pos_embed[...].astype(F32)
    residual[...] = embedded.astype(BF16)
    centre = residual[...].astype(F32)
    centre = centre - jnp.mean(centre, axis=1, keepdims=True)
    inverse = lax.rsqrt(jnp.mean(centre * centre, axis=1, keepdims=True) + 1e-06)
    inverse = jnp.broadcast_to(inverse, (tokens, lanes))
    stats = [inverse[i * lanes : (i + 1) * lanes].T[0:1] for i in range(tokens // lanes)]
    stats.append(jnp.zeros((8 - len(stats), lanes), F32))
    stats = jnp.concatenate(stats, axis=0)
    stats_send[...] = stats
    stats_got[me] = stats

    def stats_copy(source, peer):
        return remote(
            stats_send,
            stats_got.at[source],
            stats_send_sem.at[peer],
            stats_recv_sem.at[source],
            ctx=peer,
        )

    each_peer(lambda peer: stats_copy(me, peer).start())

    twin_corner = twin + 1 - 2 * my_side
    for step in range(pairs - 1):
        source = 2 * pair_at(step) + my_side
        blocks_relay(source, 0).wait_recv()

        @pl.when(source != twin_corner)
        def _():
            blocks_relay(source, pairs + 1 + step).start()

    relay_first(*range(1, n // 2))
    for step in range(pairs - 1):
        source = 2 * pair_at(step) + 1 - my_side

        @pl.when(source != corner)
        def _():
            blocks_relay(source, 0).wait_recv()

    for mask in range(2, n):
        spread_windows(partner(me, mask, n))
    lag = n // 2 - 2
    for mask in range(1, n + lag):
        if n // 2 <= mask < n:
            relay_first(mask)
        if mask > lag:
            relay_second(mask - lag)

    each_peer(lambda peer: stats_copy(peer, peer).wait_recv())

    def arrived(source):
        relay(1, source, near, near).wait_recv()
        relay(3, source, diagonal, near).wait_recv()

    each_peer(arrived)

    scales = (1.0 / head_size**0.5, 1.0, 1.0)
    for t in range(n):
        nothing = jnp.zeros((tokens, 256), BF16)
        patches = patches_of(
            windows[t - 1] if t > 0 else nothing,
            windows[t],
            windows[t + 1] if t < n - 1 else nothing,
        )
        result = jnp.dot(patches, mixing, preferred_element_type=F32) + part[t].astype(F32)
        inverse = jnp.concatenate(
            [
                jnp.broadcast_to(stats_got[t, i : i + 1, :], (lanes, lanes)).T
                for i in range(tokens // lanes)
            ],
            axis=0,
        )
        for kind, scale in enumerate(scales):
            columns = slice(kind * lanes, (kind + 1) * lanes)
            rows = result[:, columns] * inverse + shift[:, columns]
            if kind == 0:
                query[t] = (rows * scale).astype(BF16)
            elif kind == 1:
                key[:, t * tokens : (t + 1) * tokens] = rows.T.astype(BF16)
            else:
                value_wide[t * tokens : (t + 1) * tokens, 0:lanes] = rows.astype(BF16)
    keys_total = n * tokens
    value_wide[:, lanes:] = jnp.ones((keys_total, lanes), BF16)

    rows = min(tokens, ROWS)
    halves = range(tokens // rows)

    def mixed_copy(half, source, peer):
        return remote(
            mixed_send.at[half, peer],
            mixed_got.at[half, source],
            mixed_send_sem.at[half, peer],
            mixed_recv_sem.at[half, source],
            ctx=peer,
        )

    batch = n // 2

    def attend(turn, carry):
        half = lax.rem(turn, len(halves))
        peers = [partner(me, n - 1 - turn // len(halves) * batch - i, n) for i in range(batch)]
        mine_rows = pl.ds(pl.multiple_of(half * rows, rows), rows)
        lane = iota((rows, lanes), 1) // head_size
        for peer in peers:
            picked = query[peer, mine_rows, :]
            mixed = None
            for head in range(local_heads):
                mine = jnp.where(lane == head, picked, jnp.zeros_like(picked))
                scores = jnp.dot(mine, key[...], preferred_element_type=F32)
                weight = jnp.exp(scores - jnp.max(scores, axis=1, keepdims=True))
                product = jnp.dot(
                    weight.astype(BF16), value_wide[...], preferred_element_type=F32
                )
                product = product[:, 0:lanes] / product[:, lanes:]
                mixed = product if mixed is None else jnp.where(lane == head, product, mixed)
            mixed_send[half, peer] = mixed.astype(BF16)
        for i, peer in enumerate(peers):
            if i < batch - 1:
                mixed_copy(half, me, peer).start()
            else:

                @pl.when(turn < len(halves))
                def _():
                    mixed_copy(half, me, peer).start()

        return carry

    lax.fori_loop(0, 2 * len(halves), attend, 0)
    for half in halves:
        mixed_got[half, me] = mixed_send[half, me]

    hidden_width = w_fc1.shape[1]
    tile = math.gcd(hidden_width, 1024)
    for copy in weights:
        copy.wait()
    for half in halves:
        each_peer(lambda peer: mixed_copy(half, peer, peer).wait_recv())
    attended = jnp.concatenate(
        [
            jnp.concatenate([mixed_got[half, piece] for piece in range(n)], axis=1)
            for half in halves
        ],
        axis=0,
    )
    stream = (
        residual[...].astype(F32)
        + jnp.dot(attended, w_out[...], preferred_element_type=F32)
        + out_bias[...]
    ).astype(BF16)
    stream = stream.astype(F32)
    normed[...] = norm_rows(stream, ln2_gain[...], ln2_bias[...]).astype(BF16)
    total[...] = stream + fc2_bias[...]
    for start in range(0, hidden_width, tile):
        columns = slice(start, start + tile)
        hidden = jnp.dot(normed[...], w_fc1[:, columns], preferred_element_type=F32)
        hidden = hidden + fc1_bias[:, columns]
        hidden = 0.5 * hidden * (1.0 + lax.erf(hidden * math.sqrt(0.5)))
        total[...] += jnp.dot(hidden.astype(BF16), w_fc2[columns, :], preferred_element_type=F32)
    encoded[...] = total[...].astype(BF16)

    def finish(peer):
        sum_copy(me, peer).wait_send()
        stats_copy(me, peer).wait_send()
        part_copy(me, peer).wait_send()
        for half in halves:
            mixed_copy(half, me, peer).wait_send()
        relay(1, peer, replica, near).wait_send()
        relay(2, peer, replica, across).wait_send()
        relay(3, peer, across, near).wait_send()

    each_peer(finish)
    for step in range(pairs - 1):
        source = 2 * pair_at(step) + my_side
        blocks_copy(step, source).wait_send()

        @pl.when(source != twin_corner)
        def _():
            blocks_relay(source, pairs + 1 + step).wait_send()

    blocks_copy(pairs - 1, twin).wait_send()

    @pl.when(inside == 1)
    def _():
        blocks_copy(pairs, corner).wait_send()


def shared_call(
    density,
    stem_weight,
    stem_bias,
    pos_embed,
    ln1_gain,
    ln1_bias,
    w_qkv,
    qkv_bias,
    w_out,
    out_bias,
    ln2_gain,
    ln2_bias,
    w_fc1,
    fc1_bias,
    w_fc2,
    fc2_bias,
):
    n = lax.axis_size("ctx")
    tokens, width = pos_embed.shape
    side = density.shape[1]
    vmem = pl.BlockSpec(memory_space=pltpu.VMEM)
    hbm = pl.BlockSpec(memory_space=pl.ANY)
    tables = stem_tables(side, stem_weight.shape[0])

    def line(vector):
        return vector.reshape(1, -1)

    dma = pltpu.SemaphoreType.DMA
    lanes = 128
    pairs = n // 2
    return pl.pallas_call(
        functools.partial(shared_kernel, n, (density.shape[0] * side * side) * n),
        out_shape=jax.ShapeDtypeStruct((tokens, width), BF16),
        in_specs=[
            vmem, vmem, vmem, vmem, vmem, vmem, hbm, vmem,
            hbm, vmem, vmem, vmem, hbm, vmem, hbm, vmem,
            hbm, hbm, hbm, hbm,
        ],
        out_specs=vmem,
        scratch_shapes=[
            pltpu.VMEM(w_qkv.shape, BF16),
            pltpu.VMEM(w_out.shape, BF16),
            pltpu.VMEM(w_fc1.shape, BF16),
            pltpu.VMEM(w_fc2.shape, BF16),
            *[pltpu.VMEM(table.shape, BF16) for table in tables],
            dma((4,)),
            dma((3,)),
            dma((4,)),
            pltpu.VMEM((8, lanes), F32),
            pltpu.VMEM((n, 8, lanes), F32),
            pltpu.VMEM((8, lanes), F32),
            pltpu.VMEM((n, 8, lanes), F32),
            pltpu.VMEM((tokens // 2, lanes), BF16),
            pltpu.VMEM((n, tokens // 2, lanes), BF16),
            pltpu.VMEM((n, tokens, 256), BF16),
            pltpu.VMEM((256, width), BF16),
            pltpu.VMEM((256, width), BF16),
            pltpu.VMEM((tokens, width), BF16),
            pltpu.VMEM((tokens, width), BF16),
            pltpu.VMEM((tokens, width), BF16),
            pltpu.VMEM((n, tokens // 4, 3 * lanes), BF16),
            pltpu.VMEM((n, tokens, 3 * lanes), BF16),
            pltpu.VMEM((n, tokens, lanes), BF16),
            pltpu.VMEM((lanes, n * tokens), BF16),
            pltpu.VMEM((n * tokens, 2 * lanes), BF16),
            pltpu.VMEM((tokens // ROWS, n, ROWS, lanes), BF16),
            pltpu.VMEM((tokens // ROWS, n, ROWS, lanes), BF16),
            pltpu.VMEM((tokens, width), F32),
            dma((n,)),
            dma((n,)),
            dma((n,)),
            dma((n,)),
            dma((2 * pairs + 1,)),
            dma((n,)),
            dma((4, n)),
            dma((4, n)),
            dma((tokens // ROWS, n)),
            dma((tokens // ROWS, n)),
        ],
        compiler_params=pltpu.CompilerParams(
            collective_id=1, has_side_effects=True, vmem_limit_bytes=60 * 1024 * 1024
        ),
    )(
        density,
        stem_weight,
        line(stem_bias),
        pos_embed,
        line(ln1_gain),
        line(ln1_bias),
        w_qkv,
        line(qkv_bias),
        w_out,
        line(out_bias),
        line(ln2_gain),
        line(ln2_bias),
        w_fc1,
        line(fc1_bias),
        w_fc2,
        line(fc2_bias),
        *tables,
    )


def per_device(
    density,
    stem_weight,
    stem_bias,
    pos_embed,
    ln1_gain,
    ln1_bias,
    w_qkv,
    qkv_bias,
    w_out,
    out_bias,
    ln2_gain,
    ln2_bias,
    w_fc1,
    fc1_bias,
    w_fc2,
    fc2_bias,
):
    n = lax.axis_size("ctx")
    tokens, width = pos_embed.shape
    if shares_positions(n, lax.axis_size("dp"), density, pos_embed):
        return shared_call(
            density, stem_weight, stem_bias, pos_embed, ln1_gain, ln1_bias, w_qkv, qkv_bias,
            w_out, out_bias, ln2_gain, ln2_bias, w_fc1, fc1_bias, w_fc2, fc2_bias,
        )
    hidden_width = w_fc1.shape[1]
    planes, side, _ = density.shape
    assert planes == STRIDE and tokens == (side // STRIDE) ** 2
    head_size = width // HEADS
    local_heads = max(HEADS // n, 1)
    groups = max(n // HEADS, 1)
    head_groups = HEADS // local_heads
    group_width = local_heads * head_size
    share = tokens // groups
    pair = 2 * side
    window = planes + 2
    vmem = pl.BlockSpec(memory_space=pltpu.VMEM)
    hbm = pl.BlockSpec(memory_space=pl.ANY)

    def line(vector):
        return vector.reshape(1, -1)

    dma = pltpu.SemaphoreType.DMA
    wide_shape = (n * tokens, 2 * group_width) if group_width % 128 == 0 else (16, 128)
    return pl.pallas_call(
        functools.partial(layer_kernel, n, density.size * n),
        out_shape=jax.ShapeDtypeStruct((tokens, width), BF16),
        in_specs=[
            vmem, vmem, vmem, vmem, vmem, vmem, hbm, vmem,
            hbm, vmem, vmem, vmem, hbm, vmem, hbm, vmem,
        ],
        out_specs=vmem,
        scratch_shapes=[
            pltpu.VMEM(w_qkv.shape, BF16),
            pltpu.VMEM(w_out.shape, BF16),
            pltpu.VMEM(w_fc1.shape, BF16),
            pltpu.VMEM(w_fc2.shape, BF16),
            dma((4,)),
            pltpu.VMEM((2, side, side), F32),
            pltpu.VMEM((8, 128), F32),
            pltpu.VMEM((n, 8, 128), F32),
            dma((2,)),
            dma((2,)),
            dma((n,)),
            dma((n,)),
            pltpu.VMEM((KERNEL, tokens, side), BF16),
            pltpu.VMEM((KERNEL, window * pair, 256), BF16),
            pltpu.VMEM((side, window * pair), BF16),
            pltpu.VMEM((256, width), BF16),
            pltpu.VMEM((tokens, width), BF16),
            pltpu.VMEM((tokens, width), BF16),
            pltpu.VMEM((3, head_groups, tokens, group_width), BF16),
            pltpu.VMEM((n, share, group_width), BF16),
            pltpu.VMEM((n, tokens, group_width), BF16),
            pltpu.VMEM((n, tokens, group_width), BF16),
            pltpu.VMEM(wide_shape, BF16),
            pltpu.VMEM((n, share, group_width), BF16),
            pltpu.VMEM((n, share, group_width), BF16),
            pltpu.VMEM((tokens, width), BF16),
            pltpu.VMEM((tokens, width), F32),
            dma((4, n)),
            dma((4, n)),
        ],
        compiler_params=pltpu.CompilerParams(
            collective_id=0, has_side_effects=True, vmem_limit_bytes=60 * 1024 * 1024
        ),
    )(
        density,
        stem_weight,
        line(stem_bias),
        pos_embed,
        line(ln1_gain),
        line(ln1_bias),
        w_qkv,
        line(qkv_bias),
        w_out,
        line(out_bias),
        line(ln2_gain),
        line(ln2_bias),
        w_fc1,
        line(fc1_bias),
        w_fc2,
        line(fc2_bias),
    )


def solution(mesh):
    in_specs = (P(("dp", "ctx"), None, None), P(), P(), P("ctx", None)) + (P(),) * 12
    return jax.shard_map(
        per_device,
        mesh=mesh,
        in_specs=in_specs,
        out_specs=P(("dp", "ctx"), None),
        check_vma=False,
    )
```
